8 devices in a mesh: dp: 1 (over z), tp: 2 (over y), cp: 4 (over x, core).
Axes of the slice: x: 2, y: 2, z: 1, core: 2. Of those that a mesh axis runs over, the one named last changes fastest.
Arguments:
- x_in: bfloat16 [4096, 4096], P(('dp', 'cp'))
- positions: int32 [4096], P(('dp', 'cp'))
- norm_gain: bfloat16 [4096], replicated
- w_q: bfloat16 [4096, 4096], P(None, 'tp')
- w_k: bfloat16 [4096, 1024], P(None, 'tp')
- w_v: bfloat16 [4096, 1024], P(None, 'tp')
- w_o: bfloat16 [4096, 4096], P('tp')
Outputs:
- output 1: bfloat16 [4096, 4096], P(('dp', 'cp'))
- output 2: bfloat16 [4096, 8, 128], P(('dp', 'cp'), 'tp')
- output 3: bfloat16 [4096, 8, 128], P(('dp', 'cp'), 'tp')
All inputs are finite; a program needn't handle non-finite values.
Results may differ from the reference program's by a relative error of at most 0.00960483.
Values are sent between devices in bfloat16 or wider.
A program may use at most 1 GiB of HBM per device.

```python
import math
import jax
import jax.numpy as jnp
from jax import lax

MODEL_DIM = 4096
Q_HEADS = 32
KV_HEADS = 8
HEAD_DIM = 128
SEQ_LEN = 4096
CP_SIZE = 4


def rope_freqs():
    exponent = jnp.arange(0, HEAD_DIM, 2).astype(jnp.float32) / HEAD_DIM
    base_freq = 1.0 / (500000.0 ** exponent)
    wave_len = 2.0 * math.pi / base_freq
    smooth = (8192.0 / wave_len - 1.0) / 3.0
    blended = (1.0 - smooth) * base_freq / 8.0 + smooth * base_freq
    return jnp.where(wave_len < 2048.0, base_freq, jnp.where(wave_len > 8192.0, base_freq / 8.0, blended))


def apply_rope(vecs, positions, freqs):
    half_dim = HEAD_DIM // 2
    angles = positions.astype(jnp.float32)[:, None] * freqs[None, :]
    cosine = jnp.cos(angles)[:, None, :]
    sine_val = jnp.sin(angles)[:, None, :]
    vec_f32 = vecs.astype(jnp.float32)
    first_half = vec_f32[..., :half_dim]
    second_half = vec_f32[..., half_dim:]
    return jnp.concatenate([first_half * cosine - second_half * sine_val, second_half * cosine + first_half * sine_val], axis=-1).astype(jnp.bfloat16)


def setup_inputs(seed: int = 0, part: int = 0) -> dict:
    base_key = jax.random.key(seed)
    part_key = jax.random.fold_in(base_key, part)
    key_off, key_mean, key_noise = jax.random.split(part_key, 3)
    key_gain, key_q, key_k, key_v, key_o = jax.random.split(base_key, 5)
    seg_len = SEQ_LEN // (2 * CP_SIZE)
    dev_ids = jnp.arange(CP_SIZE)[:, None]
    seg_ids = jnp.concatenate([dev_ids, 2 * CP_SIZE - 1 - dev_ids], axis=1).reshape(2 * CP_SIZE)
    glob_idx = (seg_ids[:, None] * seg_len + jnp.arange(seg_len)[None, :]).reshape(SEQ_LEN)
    offset = jax.random.randint(key_off, (), 0, 4096)
    positions = (glob_idx + offset).astype(jnp.int32)
    seg_means = jax.random.normal(key_mean, (2 * CP_SIZE, MODEL_DIM), jnp.float32)
    row_means = jnp.repeat(seg_means[seg_ids], seg_len, axis=0)
    tok_noise = jax.random.normal(key_noise, (SEQ_LEN, MODEL_DIM), jnp.float32)
    x_in = (0.5 * (row_means + 0.5 * tok_noise)).astype(jnp.bfloat16)
    norm_gain = (1.0 + 0.3 * jax.random.normal(key_gain, (MODEL_DIM,), jnp.float32)).astype(jnp.bfloat16)
    in_scale = 1.0 / math.sqrt(MODEL_DIM)
    w_q = (jax.random.normal(key_q, (MODEL_DIM, Q_HEADS * HEAD_DIM), jnp.float32) * (2.0 * in_scale)).astype(jnp.bfloat16)
    w_k = (jax.random.normal(key_k, (MODEL_DIM, KV_HEADS * HEAD_DIM), jnp.float32) * in_scale).astype(jnp.bfloat16)
    w_v = (jax.random.normal(key_v, (MODEL_DIM, KV_HEADS * HEAD_DIM), jnp.float32) * in_scale).astype(jnp.bfloat16)
    w_o = (jax.random.normal(key_o, (Q_HEADS * HEAD_DIM, MODEL_DIM), jnp.float32) * (2.0 / math.sqrt(Q_HEADS * HEAD_DIM))).astype(jnp.bfloat16)
    return dict(x_in=x_in, positions=positions, norm_gain=norm_gain, w_q=w_q, w_k=w_k, w_v=w_v, w_o=w_o)


def reference(x_in, positions, norm_gain, w_q, w_k, w_v, w_o):
    seq_rows = x_in.shape[0]
    group_size = Q_HEADS // KV_HEADS
    x_f32 = x_in.astype(jnp.float32)
    normed = x_f32 * lax.rsqrt(jnp.mean(x_f32 * x_f32, axis=-1, keepdims=True) + 1e-5)
    hidden = (normed * norm_gain.astype(jnp.float32)[None, :]).astype(jnp.bfloat16)
    freqs = rope_freqs()
    queries = jnp.dot(hidden, w_q, preferred_element_type=jnp.float32).astype(jnp.bfloat16).reshape(seq_rows, Q_HEADS, HEAD_DIM)
    keys = jnp.dot(hidden, w_k, preferred_element_type=jnp.float32).astype(jnp.bfloat16).reshape(seq_rows, KV_HEADS, HEAD_DIM)
    values = jnp.dot(hidden, w_v, preferred_element_type=jnp.float32).astype(jnp.bfloat16).reshape(seq_rows, KV_HEADS, HEAD_DIM)
    queries = apply_rope(queries, positions, freqs)
    keys = apply_rope(keys, positions, freqs)
    q_blk = seq_rows
    while q_blk % 2 == 0 and q_blk > 8 and q_blk * seq_rows * Q_HEADS > 2 ** 24:
        q_blk = q_blk // 2
    n_blocks = seq_rows // q_blk
    q_grouped = queries.reshape(n_blocks, q_blk, KV_HEADS, group_size, HEAD_DIM)
    q_pos = positions.reshape(n_blocks, q_blk)
    keys_f32 = keys.astype(jnp.float32)
    values_f32 = values.astype(jnp.float32)
    score_scale = 1.0 / math.sqrt(HEAD_DIM)

    def attend(block):
        q_part, pos_part = block
        scores = jnp.einsum('qhgd,thd->qhgt', q_part.astype(jnp.float32), keys_f32) * score_scale
        keep_mask = positions[None, None, None, :] <= pos_part[:, None, None, None]
        scores = jnp.where(keep_mask, scores, -jnp.inf)
        prob_bf = jax.nn.softmax(scores, axis=-1).astype(jnp.bfloat16)
        attn_out = jnp.einsum('qhgt,thd->qhgd', prob_bf.astype(jnp.float32), values_f32)
        return attn_out.astype(jnp.bfloat16)

    o_blocks = lax.map(attend, (q_grouped, q_pos))
    attn = o_blocks.reshape(seq_rows, Q_HEADS * HEAD_DIM)
    y_out = (x_f32 + jnp.dot(attn, w_o, preferred_element_type=jnp.float32)).astype(jnp.bfloat16)
    return y_out, keys, values
```

```python
import math
import functools
import jax
import jax.numpy as jnp
from jax import lax
from jax.experimental import pallas as pl
from jax.experimental.pallas import tpu as pltpu
from jax.sharding import PartitionSpec as P

HEAD_DIM = 128
NORM_EPS = 1e-5
SCALE_LOG2 = (1.0 / math.sqrt(HEAD_DIM)) * math.log2(math.e)
MIB = 1024 * 1024


def rope_freqs():
    exponent = jnp.arange(0, HEAD_DIM, 2).astype(jnp.float32) / HEAD_DIM
    base_freq = 1.0 / (500000.0 ** exponent)
    wave_len = 2.0 * math.pi / base_freq
    smooth = (8192.0 / wave_len - 1.0) / 3.0
    blended = (1.0 - smooth) * base_freq / 8.0 + smooth * base_freq
    return jnp.where(wave_len < 2048.0, base_freq, jnp.where(wave_len > 8192.0, base_freq / 8.0, blended))


def kv_kernel(x_ref, gain_ref, wk_ref, wv_ref, cos_ref, sin_ref, h_ref, k_ref, v_ref, kh_ref, vt_ref):
    x = x_ref[...].astype(jnp.float32)
    normed = x * lax.rsqrt(jnp.mean(x * x, axis=-1, keepdims=True) + NORM_EPS)
    h = (normed * gain_ref[...].astype(jnp.float32)).astype(jnp.bfloat16)
    h_ref[...] = h
    k = jnp.dot(h, wk_ref[...], preferred_element_type=jnp.float32).astype(jnp.bfloat16)
    v = jnp.dot(h, wv_ref[...], preferred_element_type=jnp.float32).astype(jnp.bfloat16)
    v_ref[...] = v
    for n in range(k.shape[1] // HEAD_DIM):
        cols = slice(n * HEAD_DIM, (n + 1) * HEAD_DIM)
        vec = k[:, cols].astype(jnp.float32)
        rot = (vec * cos_ref[...] + pltpu.roll(vec, HEAD_DIM // 2, 1) * sin_ref[...]).astype(jnp.bfloat16)
        k_ref[:, cols] = rot
        kh_ref[n] = rot
        vt_ref[n] = v[:, cols].astype(jnp.float32).T.astype(jnp.bfloat16)


def project_kv(x_in, norm_gain, w_k, w_v, cos_full, sin_full):
    rows, dim = x_in.shape
    cols = w_k.shape[1]
    n_kv = cols // HEAD_DIM
    blk = 256
    row_blk = lambda i: (i, 0)
    whole = lambda i: (0, 0)
    return pl.pallas_call(
        kv_kernel,
        grid=(rows // blk,),
        in_specs=[
            pl.BlockSpec((blk, dim), row_blk),
            pl.BlockSpec((1, dim), whole),
            pl.BlockSpec((dim, cols), whole),
            pl.BlockSpec((dim, cols), whole),
            pl.BlockSpec((blk, HEAD_DIM), row_blk),
            pl.BlockSpec((blk, HEAD_DIM), row_blk),
        ],
        out_specs=[
            pl.BlockSpec((blk, dim), row_blk),
            pl.BlockSpec((blk, cols), row_blk),
            pl.BlockSpec((blk, cols), row_blk),
            pl.BlockSpec((n_kv, blk, HEAD_DIM), lambda i: (0, i, 0)),
            pl.BlockSpec((n_kv, HEAD_DIM, blk), lambda i: (0, 0, i)),
        ],
        out_shape=[
            jax.ShapeDtypeStruct((rows, dim), jnp.bfloat16),
            jax.ShapeDtypeStruct((rows, cols), jnp.bfloat16),
            jax.ShapeDtypeStruct((rows, cols), jnp.bfloat16),
            jax.ShapeDtypeStruct((n_kv, rows, HEAD_DIM), jnp.bfloat16),
            jax.ShapeDtypeStruct((n_kv, HEAD_DIM, rows), jnp.bfloat16),
        ],
        compiler_params=pltpu.CompilerParams(vmem_limit_bytes=56 * MIB),
        cost_estimate=pl.CostEstimate(flops=4 * rows * dim * cols, bytes_accessed=30 * MIB, transcendentals=0),
        name="project_kv",
    )(x_in, norm_gain.reshape(1, dim), w_k, w_v, cos_full, sin_full)


def q_kernel(h_ref, w_ref, cos_ref, sin_ref, qt_ref):
    half = HEAD_DIM // 2
    q = jnp.dot(h_ref[...], w_ref[...], preferred_element_type=jnp.float32).astype(jnp.bfloat16)
    for n in range(q.shape[1] // HEAD_DIM):
        vec = q[:, n * HEAD_DIM:(n + 1) * HEAD_DIM].astype(jnp.float32).T
        a = vec[:half]
        b = vec[half:]
        qt_ref[n * HEAD_DIM:n * HEAD_DIM + half] = (a * cos_ref[...] - b * sin_ref[...]).astype(jnp.bfloat16)
        qt_ref[n * HEAD_DIM + half:(n + 1) * HEAD_DIM] = (b * cos_ref[...] + a * sin_ref[...]).astype(jnp.bfloat16)


def project_q(hidden, w_q, cos_t, sin_t):
    rows, dim = hidden.shape
    cols = w_q.shape[1]
    tile = 512
    half = HEAD_DIM // 2
    return pl.pallas_call(
        q_kernel,
        grid=(cols // tile,),
        in_specs=[
            pl.BlockSpec((rows, dim), lambda j: (0, 0)),
            pl.BlockSpec((dim, tile), lambda j: (0, j)),
            pl.BlockSpec((half, rows), lambda j: (0, 0)),
            pl.BlockSpec((half, rows), lambda j: (0, 0)),
        ],
        out_specs=pl.BlockSpec((tile, rows), lambda j: (j, 0)),
        out_shape=jax.ShapeDtypeStruct((cols, rows), jnp.bfloat16),
        compiler_params=pltpu.CompilerParams(vmem_limit_bytes=56 * MIB),
        cost_estimate=pl.CostEstimate(flops=2 * rows * dim * cols, bytes_accessed=30 * MIB, transcendentals=0),
        name="project_q",
    )(hidden, w_q, cos_t, sin_t)


def attn_kernel(qt_ref, *refs):
    k_refs = refs[0:8:2]
    v_refs = refs[1:8:2]
    o_ref, o_perm_ref = refs[8:10]
    m_ref, l_ref, acc_ref = refs[10:13]
    seg = k_refs[0].shape[1] // 2
    heads = qt_ref.shape[0] // HEAD_DIM
    me = lax.axis_index("cp")

    m_ref[...] = jnp.full_like(m_ref, -1e30)
    l_ref[...] = jnp.zeros_like(l_ref)
    acc_ref[...] = jnp.zeros_like(acc_ref)
    causal = lax.broadcasted_iota(jnp.int32, (seg, seg), 0) <= lax.broadcasted_iota(jnp.int32, (seg, seg), 1)

    def block(q_half, k, vt, diagonal):
        q_cols = pl.ds(pl.multiple_of(q_half * seg, seg), seg)
        for n in range(heads):
            qt = qt_ref[n * HEAD_DIM:(n + 1) * HEAD_DIM, q_cols]
            s = jnp.dot(k, qt, preferred_element_type=jnp.float32)
            if diagonal:
                s = jnp.where(causal, s, -1e30)
            m_old = m_ref[q_half, n:n + 1, :]
            m_new = jnp.maximum(m_old, jnp.max(s, axis=0, keepdims=True))
            alpha = jnp.exp2((m_old - m_new) * SCALE_LOG2)
            p = jnp.exp2(s * SCALE_LOG2 - m_new * SCALE_LOG2)
            m_ref[q_half, n:n + 1, :] = m_new
            l_ref[q_half, n:n + 1, :] = l_ref[q_half, n:n + 1, :] * alpha + jnp.sum(p, axis=0, keepdims=True)
            rows = slice(n * HEAD_DIM, (n + 1) * HEAD_DIM)
            acc_ref[q_half, rows, :] = acc_ref[q_half, rows, :] * alpha + jnp.dot(
                vt, p.astype(jnp.bfloat16), preferred_element_type=jnp.float32)

    low = slice(0, seg)
    high = slice(seg, 2 * seg)
    block(0, k_refs[0][0, low, :], v_refs[0][0, :, low], True)
    block(1, k_refs[0][0, high, :], v_refs[0][0, :, high], True)
    block(1, k_refs[0][0, low, :], v_refs[0][0, :, low], False)
    for flip in (1, 2, 3):
        k_ref, v_ref = k_refs[flip], v_refs[flip]
        block(1, k_ref[0, low, :], v_ref[0, :, low], False)
        half = jnp.where(jnp.bitwise_xor(me, flip) < me, 0, 1)
        keys = pl.ds(pl.multiple_of(half * seg, seg), seg)
        block(half, k_ref[0, keys, :], v_ref[0, :, keys], False)

    for q_half in (0, 1):
        for n in range(heads):
            rows = slice(n * HEAD_DIM, (n + 1) * HEAD_DIM)
            o = acc_ref[q_half, rows, :] / l_ref[q_half, n:n + 1, :]
            o = o.T.astype(jnp.bfloat16)
            out_rows = slice(q_half * seg, (q_half + 1) * seg)
            o_ref[out_rows, rows] = o
            slot = jnp.bitwise_xor(me, n) * HEAD_DIM
            o_perm_ref[out_rows, pl.ds(pl.multiple_of(slot, HEAD_DIM), HEAD_DIM)] = o


def attend(q_t, group, index, sources, group_size):
    rows = q_t.shape[1]
    width = group_size * HEAD_DIM
    seg = rows // 2
    in_specs = [pl.BlockSpec((width, rows), lambda _: (group, 0))]
    operands = [q_t]
    for k, v_t in sources:
        in_specs += [pl.BlockSpec((1, rows, HEAD_DIM), lambda _: (index, 0, 0)),
                     pl.BlockSpec((1, HEAD_DIM, rows), lambda _: (index, 0, 0))]
        operands += [k, v_t]
    out = jax.ShapeDtypeStruct((rows, width), jnp.bfloat16)
    return pl.pallas_call(
        attn_kernel,
        grid=(1,),
        in_specs=in_specs,
        out_specs=[pl.BlockSpec((rows, width), lambda _: (0, 0))] * 2,
        out_shape=[out, out],
        scratch_shapes=[
            pltpu.VMEM((2, 8, seg), jnp.float32),
            pltpu.VMEM((2, 8, seg), jnp.float32),
            pltpu.VMEM((2, width, seg), jnp.float32),
        ],
        compiler_params=pltpu.CompilerParams(vmem_limit_bytes=40 * MIB),
        cost_estimate=pl.CostEstimate(flops=2 * 9 * seg * seg * 4 * width, bytes_accessed=8 * MIB, transcendentals=0),
        name="attend",
    )(*operands)


def out_own_kernel(x_ref, o0, o1, o2, o3, w_ref, acc_ref):
    o = jnp.concatenate([o0[...], o1[...], o2[...], o3[...]], axis=1)
    acc_ref[...] = x_ref[...].astype(jnp.float32) + jnp.dot(o, w_ref[...], preferred_element_type=jnp.float32)


def out_own(x_in, outs, w_o):
    rows, dim = x_in.shape
    width = outs[0].shape[1]
    tile = 512
    col = lambda j: (0, j)
    whole = lambda j: (0, 0)
    return pl.pallas_call(
        out_own_kernel,
        grid=(dim // tile,),
        in_specs=[pl.BlockSpec((rows, tile), col)] + [pl.BlockSpec((rows, width), whole)] * 4
        + [pl.BlockSpec((4 * width, tile), col)],
        out_specs=pl.BlockSpec((rows, tile), col),
        out_shape=jax.ShapeDtypeStruct((rows, dim), jnp.float32),
        compiler_params=pltpu.CompilerParams(vmem_limit_bytes=56 * MIB),
        cost_estimate=pl.CostEstimate(flops=2 * rows * dim * 4 * width, bytes_accessed=44 * MIB, transcendentals=0),
        name="out_own",
    )(x_in, *outs, w_o)


def out_other_kernel(acc_ref, *refs):
    out_ref = refs[-1]
    total = acc_ref[...]
    for n in range(len(refs) // 5):
        o_ref = refs[5 * n]
        w = jnp.concatenate([r[...] for r in refs[5 * n + 1:5 * n + 5]], axis=0)
        total = total + jnp.dot(o_ref[...], w, preferred_element_type=jnp.float32)
    out_ref[...] = total.astype(out_ref.dtype)


def out_other(acc, parts, dtype):
    rows, dim = acc.shape
    tile = 512
    col = lambda j: (0, j)
    whole = lambda j: (0, 0)
    in_specs = [pl.BlockSpec((rows, tile), col)]
    operands = [acc]
    for o, blocks in parts:
        in_specs += [pl.BlockSpec(o.shape, whole)] + [pl.BlockSpec((b.shape[0], tile), col) for b in blocks]
        operands += [o, *blocks]
    return pl.pallas_call(
        out_other_kernel,
        grid=(dim // tile,),
        in_specs=in_specs,
        out_specs=pl.BlockSpec((rows, tile), col),
        out_shape=jax.ShapeDtypeStruct((rows, dim), dtype),
        input_output_aliases={0: 0} if dtype == acc.dtype else {},
        compiler_params=pltpu.CompilerParams(vmem_limit_bytes=56 * MIB),
        cost_estimate=pl.CostEstimate(flops=2 * rows * dim * 512 * len(parts), bytes_accessed=36 * MIB, transcendentals=0),
        name="out_other",
    )(*operands)


def solution(mesh):
    n_cp = mesh.shape['cp']
    flip_tp = [(0, 1), (1, 0)]
    flip_core = [(i, i ^ 1) for i in range(n_cp)]
    flip_x = [(i, i ^ 2) for i in range(n_cp)]

    def over_tp(a):
        return lax.ppermute(a, 'tp', flip_tp)

    def over_x(a):
        return lax.ppermute(a, 'cp', flip_x)

    def over_core(a):
        return lax.ppermute(a, 'cp', flip_core)

    def device_fn(x_in, positions, norm_gain, w_q, w_k, w_v, w_o):
        rows, dim = x_in.shape
        kv_dev = w_k.shape[1] // HEAD_DIM
        group_size = w_q.shape[1] // HEAD_DIM // kv_dev
        width = group_size * HEAD_DIM
        me = lax.axis_index('cp')

        w_recv = []
        for g in range(kv_dev):
            piece = lax.dynamic_slice_in_dim(w_o, g * width + me * HEAD_DIM, HEAD_DIM, axis=0)
            w_recv.append(over_tp(piece))

        freqs = rope_freqs()
        angles = positions.astype(jnp.float32)[:, None] * freqs[None, :]
        cosine, sine = jnp.cos(angles), jnp.sin(angles)
        cos_full = jnp.concatenate([cosine, cosine], axis=1)
        sin_full = jnp.concatenate([-sine, sine], axis=1)

        hidden, k_flat, v_flat, k_heads, v_t = project_kv(x_in, norm_gain, w_k, w_v, cos_full, sin_full)
        n_split = 2
        per = kv_dev // n_split
        sources = []
        for c in range(n_split):
            mine = (k_heads[c * per:(c + 1) * per], v_t[c * per:(c + 1) * per])
            from_core = tuple(over_core(a) for a in mine)
            from_x = tuple(over_x(a) for a in mine)
            from_diag = tuple(over_core(a) for a in from_x)
            sources.append((mine, from_core, from_x, from_diag))

        q_t = project_q(hidden, w_q, cosine.T, sine.T)

        own, others = [], []
        for g in range(kv_dev):
            o, o_perm = attend(q_t, g, g % per, sources[g // per], group_size)
            own.append(o)
            others.append(over_tp(o_perm))

        w_blocks = []
        for g in range(kv_dev):
            r = w_recv[g]
            a = over_x(r)
            w_blocks.append((r, over_core(r), a, over_core(a)))

        acc = out_own(x_in, own, w_o)
        acc = out_other(acc, [(others[0], w_blocks[0]), (others[1], w_blocks[1])], jnp.float32)
        acc = out_other(acc, [(others[2], w_blocks[2])], jnp.float32)
        y_out = out_other(acc, [(others[3], w_blocks[3])], jnp.bfloat16)
        return y_out, k_flat.reshape(rows, kv_dev, HEAD_DIM), v_flat.reshape(rows, kv_dev, HEAD_DIM)

    row_spec = P(('dp', 'cp'), None)
    cache_spec = P(('dp', 'cp'), 'tp', None)
    return jax.shard_map(device_fn, mesh=mesh, in_specs=(row_spec, P(('dp', 'cp')), P(None), P(None, 'tp'), P(None, 'tp'), P(None, 'tp'), P('tp', None)), out_specs=(row_spec, cache_spec, cache_spec), check_vma=False)
```

```python
import math
import functools
import numpy as np
import jax
import jax.numpy as jnp
from jax import lax
from jax.experimental import pallas as pl
from jax.experimental.pallas import tpu as pltpu
from jax.sharding import PartitionSpec as P

HEAD_DIM = 128
NORM_EPS = 1e-5
SCALE_LOG2 = (1.0 / math.sqrt(HEAD_DIM)) * math.log2(math.e)
N_CP = 4
MESH = pl.DeviceIdType.MESH
BF16 = jnp.bfloat16
F32 = jnp.float32


def rope_freqs():
    exponent = np.arange(0, HEAD_DIM, 2) / HEAD_DIM
    base_freq = 1.0 / (500000.0 ** exponent)
    wave_len = 2.0 * math.pi / base_freq
    smooth = (8192.0 / wave_len - 1.0) / 3.0
    blended = (1.0 - smooth) * base_freq / 8.0 + smooth * base_freq
    freqs = np.where(wave_len < 2048.0, base_freq, np.where(wave_len > 8192.0, base_freq / 8.0, blended))
    return freqs.astype(np.float32)


def layer_kernel(x_hbm, pos_ref, freq_ref, gain_ref, wq_hbm, wk_hbm, wv_hbm, wo_hbm,
                 y_hbm, kf_hbm, vf_hbm, w1_hbm,
                 hbuf, wbuf, xbuf, kv_ref, qt_ref, s_even, s_odd, p_even, p_odd,
                 m_ref, l_ref, att_ref, acc_ref, kst_ref, vst_ref, cos_t, sin_t, cos_f, sin_f,
                 x_sem, w_sem, f_sem, y_sem,
                 wy_s, wy_r, wx_s, wx_r, wc_s, wc_r, wd_s, wd_r,
                 kc_s, kc_r, kx_s, kx_r, kd_s, kd_r, oy_s, oy_r, or_s, or_r, free_sem):
    rows, dim = hbuf.shape
    width = wk_hbm.shape[1]
    n_grp = wq_hbm.shape[1] // width
    own_cols = n_grp * width
    seg = rows // 2
    half = HEAD_DIM // 2
    blk = 256
    n_blk = rows // blk
    heads = width // HEAD_DIM
    me = lax.axis_index("cp")
    peer_y = {"tp": 1 - lax.axis_index("tp")}
    peer_c = {"cp": me + 1 - 2 * (me % 2)}
    peer_x = {"cp": (me + 2) % N_CP}
    s_refs, p_refs = (s_even, s_odd), (p_even, p_odd)

    def at(i, size):
        return pl.ds(pl.multiple_of(i * size, size), size)

    def remote(src, dst, send, recv, peer):
        return pltpu.make_async_remote_copy(src_ref=src, dst_ref=dst, send_sem=send, recv_sem=recv,
                                            device_id=peer, device_id_type=MESH)

    def w_rows(g, owner):
        return pl.ds(pl.multiple_of(g * width + owner * HEAD_DIM, HEAD_DIM), HEAD_DIM)

    other_x = (me + 2) % N_CP

    def wy(g):
        return remote(wo_hbm.at[w_rows(g, me)], w1_hbm.at[w_rows(g, me)], wy_s.at[g], wy_r.at[g], peer_y)

    def wx(g):
        return remote(w1_hbm.at[w_rows(g, me)], w1_hbm.at[w_rows(g, me)], wx_s.at[g], wx_r.at[g], peer_x)

    def wc(g):
        return remote(w1_hbm.at[w_rows(g, me)], w1_hbm.at[w_rows(g, me)], wc_s.at[g], wc_r.at[g], peer_c)

    def wd(g):
        return remote(w1_hbm.at[w_rows(g, other_x)], w1_hbm.at[w_rows(g, other_x)], wd_s.at[g], wd_r.at[g], peer_c)

    def kc():
        return remote(kv_ref.at[0], kv_ref.at[1], kc_s, kc_r, peer_c)

    def kx(n):
        return remote(kv_ref.at[0, n], kv_ref.at[2, n], kx_s.at[n], kx_r.at[n], peer_x)

    def kd(n):
        return remote(kv_ref.at[2, n], kv_ref.at[3, n], kd_s.at[n], kd_r.at[n], peer_c)

    def oy(g):
        return remote(hbuf.at[:, at(g, width)], hbuf.at[:, at(g + n_grp, width)], oy_s.at[g], oy_r.at[g], peer_y)

    def o_last(r):
        g = n_grp - 1
        return remote(hbuf.at[at(r, blk), at(g, width)], hbuf.at[at(r, blk), at(g + n_grp, width)],
                      or_s.at[r], or_r.at[r], peer_y)

    def x_in(r):
        return pltpu.make_async_copy(x_hbm.at[at(r, blk)], xbuf.at[r % 2], x_sem.at[r % 2])

    def q_in(g):
        return pltpu.make_async_copy(wq_hbm.at[:, at(g, width)], wbuf.at[g % 2], w_sem.at[g % 2])

    def o_tile(j):
        return wbuf.at[(j % 4) // 2, at(j % 2, own_cols)]

    def o_in(j):
        return pltpu.make_async_copy(wo_hbm.at[:, at(j, width)], o_tile(j), w_sem.at[j % 4])

    n_tile = dim // width

    def w1_in(g, j):
        return pltpu.make_async_copy(w1_hbm.at[at(g, width), at(j, width)], wbuf.at[g % 2, at(j, width)], f_sem.at[g % 2, j])

    def y_out(r):
        return pltpu.make_async_copy(xbuf.at[r % 2], y_hbm.at[at(r, blk)], y_sem.at[r % 2])

    k_in = pltpu.make_async_copy(wk_hbm, wbuf.at[0], w_sem.at[0])
    v_in = pltpu.make_async_copy(wv_hbm, wbuf.at[1], w_sem.at[1])
    k_out = pltpu.make_async_copy(kst_ref, kf_hbm, y_sem.at[0])
    v_out = pltpu.make_async_copy(vst_ref, vf_hbm, y_sem.at[1])

    x_in(0).start()
    k_in.start()
    x_in(1).start()
    v_in.start()
    barrier = pltpu.get_barrier_semaphore()
    for peer in (peer_y, peer_c, peer_x):
        pl.semaphore_signal(barrier, inc=1, device_id=peer, device_id_type=MESH)
    pl.semaphore_wait(barrier, 3)
    wy(0).start()
    wy(1).start()

    def trig(c, carry):
        cols = at(c, blk)
        angle = freq_ref[...] * pos_ref[:, cols].astype(F32)
        turns = jnp.floor(angle * (0.5 / math.pi) + 0.5)
        angle = ((angle - turns * 6.28125) - turns * 1.9350051879882812e-03) - turns * 3.0199159819e-07
        cosine, sine = jnp.cos(angle), jnp.sin(angle)
        cos_t[:, cols] = cosine
        sin_t[:, cols] = sine
        cos_f[cols, :] = jnp.concatenate([cosine, cosine], axis=0).T
        sin_f[cols, :] = jnp.concatenate([-sine, sine], axis=0).T
        return carry

    lax.fori_loop(0, n_blk, trig, 0)

    k_in.wait()

    def norm_k(r, carry):
        x_in(r).wait()
        rws = at(r, blk)
        x = xbuf[r % 2].astype(F32)
        acc_ref[rws, :] = x
        normed = x * lax.rsqrt(jnp.mean(x * x, axis=-1, keepdims=True) + NORM_EPS)
        h = (normed * gain_ref[...].astype(F32)).astype(BF16)
        hbuf[rws, :] = h

        @pl.when(r < n_blk - 2)
        def _():
            x_in(r + 2).start()

        k = jnp.dot(h, wbuf[0], preferred_element_type=F32).astype(BF16)
        for n in range(heads):
            vec = k[:, n * HEAD_DIM:(n + 1) * HEAD_DIM].astype(F32)
            rot = (vec * cos_f[rws, :] + pltpu.roll(vec, half, 1) * sin_f[rws, :]).astype(BF16)
            kst_ref[rws, n * HEAD_DIM:(n + 1) * HEAD_DIM] = rot
            kv_ref[0, n, 0, rws, :] = rot
        return carry

    lax.fori_loop(0, n_blk, norm_k, 0)
    q_in(0).start()
    v_in.wait()

    def proj_v(r, carry):
        rws = at(r, blk)
        v = jnp.dot(hbuf[rws, :], wbuf[1], preferred_element_type=F32).astype(BF16)
        vst_ref[rws, :] = v
        for n in range(heads):
            for b in range(blk // HEAD_DIM):
                square = v[b * HEAD_DIM:(b + 1) * HEAD_DIM, n * HEAD_DIM:(n + 1) * HEAD_DIM].astype(F32).T.astype(BF16)
                kv_ref[0, n, 1, pl.ds(pl.multiple_of(r * blk + b * HEAD_DIM, HEAD_DIM), HEAD_DIM), :] = square
        return carry

    lax.fori_loop(0, n_blk, proj_v, 0)
    q_in(1).start()

    def proj_q(g, carry):
        q_in(g).wait()

        def rows_q(r, inner):
            rws = at(r, blk)
            q = jnp.dot(hbuf[rws, :], wbuf[g % 2], preferred_element_type=F32).astype(BF16)
            for n in range(heads):
                vec = q[:, n * HEAD_DIM:(n + 1) * HEAD_DIM].astype(F32).T
                a, b = vec[:half], vec[half:]
                out = jnp.concatenate([a * cos_t[:, rws] - b * sin_t[:, rws], b * cos_t[:, rws] + a * sin_t[:, rws]], axis=0)
                qt_ref[pl.ds(pl.multiple_of(g * width + n * HEAD_DIM, HEAD_DIM), HEAD_DIM), rws] = out.astype(BF16)

            @pl.when(jnp.logical_and(g == 0, r == 0))
            def _():
                kc().start()
                kx(0).start()
                k_out.start()
                v_out.start()
            return inner

        lax.fori_loop(0, n_blk, rows_q, 0)

        @pl.when(g < n_grp - 2)
        def _():
            q_in(g + 2).start()

        @pl.when(g == 1)
        def _():
            kx(1).start()
        return carry

    lax.fori_loop(0, n_grp, proj_q, 0)
    kx(2).start()
    pl.semaphore_signal(free_sem, inc=1, device_id=peer_y, device_id_type=MESH)
    for j in range(4):
        o_in(j).start()
    kc().wait()
    k_out.wait()
    v_out.wait()

    def attention(g, outer):
        kx(g).wait_recv()
        kd(g).start()

        @pl.when(g == 1)
        def _():
            kx(3).start()

        m_ref[...] = jnp.full_like(m_ref, -1e30)
        l_ref[...] = jnp.zeros_like(l_ref)
        att_ref[...] = jnp.zeros_like(att_ref)

        def scores(q_half, src, k_half, n, slot, diagonal):
            k = kv_ref[src, g, 0, at(k_half, seg), :]
            q = qt_ref[pl.ds(pl.multiple_of(g * width + n * HEAD_DIM, HEAD_DIM), HEAD_DIM), at(q_half, seg)]
            s = jnp.dot(k, q, preferred_element_type=F32)
            if diagonal:
                keep = lax.broadcasted_iota(jnp.int32, (seg, seg), 0) <= lax.broadcasted_iota(jnp.int32, (seg, seg), 1)
                s = jnp.where(keep, s, -1e30)
            s_refs[slot][...] = s
            return jnp.max(s.reshape(seg // 8, 8, seg), axis=0)

        def soften(q_half, n, slot, top):
            chunk = 64
            m_old = m_ref[q_half, n:n + 1, :]
            m_new = jnp.maximum(m_old, jnp.max(top, axis=0, keepdims=True))
            alpha = jnp.exp2((m_old - m_new) * SCALE_LOG2)
            shift = jnp.broadcast_to(m_new * SCALE_LOG2, (8, seg))
            m_ref[q_half, n:n + 1, :] = m_new
            total = jnp.zeros((8, seg), F32)
            for c in range(0, seg, chunk):
                s = s_refs[slot][c:c + chunk, :].reshape(chunk // 8, 8, seg)
                p = jnp.exp2(s * SCALE_LOG2 - shift[None])
                total = total + jnp.sum(p, axis=0)
                p_refs[slot][c:c + chunk, :] = p.reshape(chunk, seg).astype(BF16)
            l_ref[q_half, n:n + 1, :] = l_ref[q_half, n:n + 1, :] * alpha + jnp.sum(total, axis=0, keepdims=True)
            return alpha

        def weigh(q_half, src, k_half, n, slot, alpha):
            v_t = jnp.concatenate([kv_ref[src, g, 1, pl.ds(pl.multiple_of(k_half * seg + b, HEAD_DIM), HEAD_DIM), :]
                                   for b in range(0, seg, HEAD_DIM)], axis=1)
            rws = slice(n * HEAD_DIM, (n + 1) * HEAD_DIM)
            att_ref[q_half, rws, :] = att_ref[q_half, rws, :] * alpha + jnp.dot(
                v_t, p_refs[slot][...], preferred_element_type=F32)

        def block(q_half, src, k_half, top, following):
            previous = None
            for n in range(heads):
                if n + 1 < heads:
                    top_next = scores(q_half, src, k_half, n + 1, (n + 1) % 2, following is None)
                else:
                    top_next = None if following is None else scores(*following, 0, 0, False)
                alpha = soften(q_half, n, n % 2, top)
                if previous is not None:
                    weigh(*previous)
                previous = (q_half, src, k_half, n, n % 2, alpha)
                top = top_next
            weigh(*previous)
            return top

        def place(step):
            src = (step + 1) // 2
            near = 1 - src // 2
            lower = near * (me % 2) + (1 - near) * (me // 2)
            free = (1 - step % 2) * ((step + 6) // 7)
            return 1 - free * lower, src, free * (1 - lower)

        def on_diagonal(side, carry):
            block(side, 0, side, scores(side, 0, side, 0, 0, True), None)
            return carry

        lax.fori_loop(0, 2, on_diagonal, 0)
        kd(g).wait_recv()
        n_steps = 7

        def step_body(step, top):
            @pl.when(jnp.logical_and(g == 0, step == 5))
            def _():
                wy(2).start()
                wy(3).start()

            @pl.when(jnp.logical_and(g == 1, step == 2))
            def _():
                for w in (0, 1):
                    wy(w).wait_recv()
                    wx(w).start()
                    wc(w).start()

            @pl.when(jnp.logical_and(g == 3, step == 4))
            def _():
                pl.semaphore_wait(free_sem, 1)
                oy(0).start()
                oy(1).start()

            return block(*place(step), top, place(jnp.minimum(step + 1, n_steps - 1)))

        lax.fori_loop(0, n_steps, step_body, scores(*place(0), 0, 0, False))

        def write(q_half, carry):
            for n in range(heads):
                o = (att_ref[q_half, n * HEAD_DIM:(n + 1) * HEAD_DIM, :] / l_ref[q_half, n:n + 1, :]).T.astype(BF16)
                hbuf[at(q_half, seg), pl.ds(pl.multiple_of(g * width + n * HEAD_DIM, HEAD_DIM), HEAD_DIM)] = o
            return carry

        lax.fori_loop(0, 2, write, 0)
        return outer

    lax.fori_loop(0, n_grp, attention, 0)

    def out_own(j, carry):
        o_in(j).wait()

        def add(r, inner):
            acc_ref[at(r, blk), at(j, width)] += jnp.dot(hbuf[at(r, blk), 0:own_cols], o_tile(j)[...], preferred_element_type=F32)
            return inner

        lax.fori_loop(0, n_blk, add, 0)

        @pl.when(j < n_tile - 4)
        def _():
            o_in(j + 4).start()

        @pl.when(j == 1)
        def _():
            for w in (2, 3):
                wy(w).wait_recv()
                wx(w).start()
                wc(w).start()

        @pl.when(j == 5)
        def _():
            for w in (0, 1):
                wx(w).wait_recv()
                wd(w).start()

        @pl.when(j == 6)
        def _():
            oy(2).start()
        return carry

    lax.fori_loop(0, n_tile, out_own, 0)

    def load_group(g):
        wc(g).wait_recv()
        wd(g).wait_recv()
        for j in range(n_tile):
            w1_in(g, j).start()

    def add_group(g, r):
        def add(j, carry):
            acc_ref[at(r, blk), at(j, width)] += jnp.dot(
                hbuf[at(r, blk), at(g + n_grp, width)], wbuf[g % 2, at(j, width)], preferred_element_type=F32)
            return carry

        lax.fori_loop(0, n_tile, add, 0)

    def add_rows(g):
        def body(r, carry):
            add_group(g, r)
            return carry

        lax.fori_loop(0, n_blk, body, 0)

    load_group(0)
    load_group(1)
    oy(0).wait_recv()
    o_last(0).start()
    for j in range(n_tile):
        w1_in(0, j).wait()
    add_rows(0)
    oy(1).wait_recv()
    o_last(1).start()
    for w in (2, 3):
        wx(w).wait_recv()
        wd(w).start()
    for j in range(n_tile):
        w1_in(1, j).wait()
    add_rows(1)
    load_group(2)
    load_group(3)
    o_last(2).start()
    oy(2).wait_recv()
    for j in range(n_tile):
        w1_in(2, j).wait()
    add_rows(2)
    o_last(3).start()
    for j in range(n_tile):
        w1_in(3, j).wait()

    def finish(r, carry):
        o_last(r).wait_recv()
        add_group(n_grp - 1, r)

        @pl.when(r >= 2)
        def _():
            y_out(r - 2).wait()

        xbuf[r % 2] = acc_ref[at(r, blk), :].astype(BF16)
        y_out(r).start()
        return carry

    lax.fori_loop(0, n_blk, finish, 0)
    y_out(n_blk - 2).wait()
    y_out(n_blk - 1).wait()

    for n in range(4):
        kx(n).wait_send()
        kd(n).wait_send()
        wy(n).wait_send()
        wx(n).wait_send()
        wc(n).wait_send()
        wd(n).wait_send()
        o_last(n).wait_send()
    for g in range(3):
        oy(g).wait_send()


def write_kernel(y_ref, k_ref, v_ref, y_out, k_out, v_out):
    y_out[...] = y_ref[...]
    for n in range(k_out.shape[1]):
        k_out[:, n, :] = k_ref[:, n * HEAD_DIM:(n + 1) * HEAD_DIM]
        v_out[:, n, :] = v_ref[:, n * HEAD_DIM:(n + 1) * HEAD_DIM]


def solution(mesh):
    def device_fn(x_in, positions, norm_gain, w_q, w_k, w_v, w_o):
        rows, dim = x_in.shape
        cols = w_k.shape[1]
        kv_dev = cols // HEAD_DIM
        seg = rows // 2
        half = HEAD_DIM // 2
        hbm = pl.BlockSpec(memory_space=pl.ANY)
        vmem = pl.BlockSpec(memory_space=pltpu.VMEM)
        dma = pltpu.SemaphoreType.DMA
        y_raw, k_flat, v_flat, _ = pl.pallas_call(
            layer_kernel,
            in_specs=[hbm, vmem, vmem, vmem, hbm, hbm, hbm, hbm],
            out_specs=[hbm] * 4,
            out_shape=[
                jax.ShapeDtypeStruct((rows, dim), BF16),
                jax.ShapeDtypeStruct((rows, cols), BF16),
                jax.ShapeDtypeStruct((rows, cols), BF16),
                jax.ShapeDtypeStruct(w_o.shape, BF16),
            ],
            scratch_shapes=[
                pltpu.VMEM((rows, dim), BF16),
                pltpu.VMEM((2, dim, cols), BF16),
                pltpu.VMEM((2, 256, dim), BF16),
                pltpu.VMEM((4, kv_dev, 2, rows, HEAD_DIM), BF16),
                pltpu.VMEM((w_q.shape[1], rows), BF16),
                pltpu.VMEM((seg, seg), F32),
                pltpu.VMEM((seg, seg), F32),
                pltpu.VMEM((seg, seg), BF16),
                pltpu.VMEM((seg, seg), BF16),
                pltpu.VMEM((2, 8, seg), F32),
                pltpu.VMEM((2, 8, seg), F32),
                pltpu.VMEM((2, cols, seg), F32),
                pltpu.VMEM((rows, dim), F32),
                pltpu.VMEM((rows, cols), BF16),
                pltpu.VMEM((rows, cols), BF16),
                pltpu.VMEM((half, rows), F32),
                pltpu.VMEM((half, rows), F32),
                pltpu.VMEM((rows, HEAD_DIM), F32),
                pltpu.VMEM((rows, HEAD_DIM), F32),
                dma((2,)), dma((4,)), dma((2, 8)), dma((2,)),
                dma((4,)), dma((4,)), dma((4,)), dma((4,)), dma((4,)), dma((4,)), dma((4,)), dma((4,)),
                dma, dma, dma((4,)), dma((4,)), dma((4,)), dma((4,)),
                dma((3,)), dma((3,)), dma((4,)), dma((4,)),
                pltpu.SemaphoreType.REGULAR,
            ],
            compiler_params=pltpu.CompilerParams(collective_id=0, has_side_effects=True, vmem_limit_bytes=67043328),
            name="layer",
        )(x_in, positions.reshape(1, rows), jnp.asarray(rope_freqs())[:, None], norm_gain.reshape(1, dim), w_q, w_k, w_v, w_o)
        blk = 128
        return pl.pallas_call(
            write_kernel,
            grid=(rows // blk,),
            in_specs=[pl.BlockSpec((blk, dim), lambda i: (i, 0))] + [pl.BlockSpec((blk, cols), lambda i: (i, 0))] * 2,
            out_specs=[pl.BlockSpec((blk, dim), lambda i: (i, 0))] + [pl.BlockSpec((blk, kv_dev, HEAD_DIM), lambda i: (i, 0, 0))] * 2,
            out_shape=[jax.ShapeDtypeStruct((rows, dim), BF16)] + [jax.ShapeDtypeStruct((rows, kv_dev, HEAD_DIM), BF16)] * 2,
            name="write",
        )(y_raw, k_flat, v_flat)

    row_spec = P(('dp', 'cp'), None)
    cache_spec = P(('dp', 'cp'), 'tp', None)
    return jax.shard_map(device_fn, mesh=mesh, in_specs=(row_spec, P(('dp', 'cp')), P(None), P(None, 'tp'), P(None, 'tp'), P(None, 'tp'), P('tp', None)), out_specs=(row_spec, cache_spec, cache_spec), check_vma=False)
```

```python
import math
import functools
import numpy as np
import jax
import jax.numpy as jnp
from jax import lax
from jax.experimental import pallas as pl
from jax.experimental.pallas import tpu as pltpu
from jax.sharding import PartitionSpec as P

HEAD_DIM = 128
NORM_EPS = 1e-5
SCALE_LOG2 = (1.0 / math.sqrt(HEAD_DIM)) * math.log2(math.e)
N_CP = 4
MESH = pl.DeviceIdType.MESH
BF16 = jnp.bfloat16
F32 = jnp.float32


def rope_freqs():
    exponent = np.arange(0, HEAD_DIM, 2) / HEAD_DIM
    base_freq = 1.0 / (500000.0 ** exponent)
    wave_len = 2.0 * math.pi / base_freq
    smooth = (8192.0 / wave_len - 1.0) / 3.0
    blended = (1.0 - smooth) * base_freq / 8.0 + smooth * base_freq
    freqs = np.where(wave_len < 2048.0, base_freq, np.where(wave_len > 8192.0, base_freq / 8.0, blended))
    return freqs.astype(np.float32)


def layer_kernel(x_hbm, pos_ref, freq_ref, gain_ref, wq_hbm, wk_hbm, wv_hbm, wo_hbm,
                 y_ref, kst_ref, vst_ref, w1_hbm,
                 hbuf, wbuf, kv_ref, qt_ref, s_even, s_odd, p_even, p_odd,
                 m_ref, l_ref, att_ref, acc_ref, cos_t, sin_t, gain_f,
                 x_sem, w_sem, f_sem,
                 wy_s, wy_r, wx_s, wx_r, wc_s, wc_r, wd_s, wd_r,
                 kc_s, kc_r, kx_s, kx_r, kd_s, kd_r, oy_s, oy_r, or_s, or_r, free_sem):
    rows, dim = hbuf.shape
    width = wk_hbm.shape[1]
    n_grp = wq_hbm.shape[1] // width
    own_cols = n_grp * width
    seg = rows // 2
    half = HEAD_DIM // 2
    blk = 256
    n_blk = rows // blk
    heads = width // HEAD_DIM
    me = lax.axis_index("cp")
    peer_y = {"tp": 1 - lax.axis_index("tp")}
    peer_c = {"cp": me + 1 - 2 * (me % 2)}
    peer_x = {"cp": (me + 2) % N_CP}
    s_refs, p_refs = (s_even, s_odd), (p_even, p_odd)

    def at(i, size):
        return pl.ds(pl.multiple_of(i * size, size), size)

    def remote(src, dst, send, recv, peer):
        return pltpu.make_async_remote_copy(src_ref=src, dst_ref=dst, send_sem=send, recv_sem=recv,
                                            device_id=peer, device_id_type=MESH)

    def w_rows(g, owner):
        return pl.ds(pl.multiple_of(g * width + owner * HEAD_DIM, HEAD_DIM), HEAD_DIM)

    other_x = (me + 2) % N_CP

    def wy(g):
        return remote(wo_hbm.at[w_rows(g, me)], w1_hbm.at[w_rows(g, me)], wy_s.at[g], wy_r.at[g], peer_y)

    def wx(g):
        return remote(w1_hbm.at[w_rows(g, me)], w1_hbm.at[w_rows(g, me)], wx_s.at[g], wx_r.at[g], peer_x)

    def wc(g):
        return remote(w1_hbm.at[w_rows(g, me)], w1_hbm.at[w_rows(g, me)], wc_s.at[g], wc_r.at[g], peer_c)

    def wd(g):
        return remote(w1_hbm.at[w_rows(g, other_x)], w1_hbm.at[w_rows(g, other_x)], wd_s.at[g], wd_r.at[g], peer_c)

    def kc():
        return remote(kv_ref.at[0], kv_ref.at[1], kc_s, kc_r, peer_c)

    def kx(n):
        return remote(kv_ref.at[0, n], kv_ref.at[2, n], kx_s.at[n], kx_r.at[n], peer_x)

    def kd(n):
        return remote(kv_ref.at[2, n], kv_ref.at[3, n], kd_s.at[n], kd_r.at[n], peer_c)

    def oy(g):
        return remote(hbuf.at[:, at(g, width)], hbuf.at[:, at(g + n_grp, width)], oy_s.at[g], oy_r.at[g], peer_y)

    def o_last(r):
        g = n_grp - 1
        return remote(hbuf.at[at(r, blk), at(g, width)], hbuf.at[at(r, blk), at(g + n_grp, width)],
                      or_s.at[r], or_r.at[r], peer_y)

    def x_in(r):
        return pltpu.make_async_copy(x_hbm.at[at(r, blk)], y_ref.at[at(r, blk)], x_sem.at[r])

    def q_in(g):
        return pltpu.make_async_copy(wq_hbm.at[:, at(g, width)], wbuf.at[g % 2], w_sem.at[g % 2])

    def o_tile(j):
        return wbuf.at[(j % 4) // 2, at(j % 2, own_cols)]

    def o_in(j):
        return pltpu.make_async_copy(wo_hbm.at[:, at(j, width)], o_tile(j), w_sem.at[j % 4])

    n_tile = dim // width

    def w1_in(g, j):
        return pltpu.make_async_copy(w1_hbm.at[at(g, width), at(j, width)], wbuf.at[g % 2, at(j, width)], f_sem.at[g % 2, j])

    k_in = pltpu.make_async_copy(wk_hbm, wbuf.at[0], w_sem.at[0])
    v_in = pltpu.make_async_copy(wv_hbm, wbuf.at[1], w_sem.at[1])

    x_in(0).start()
    k_in.start()
    x_in(1).start()
    v_in.start()
    x_in(2).start()
    x_in(3).start()
    barrier = pltpu.get_barrier_semaphore()
    for peer in (peer_y, peer_c, peer_x):
        pl.semaphore_signal(barrier, inc=1, device_id=peer, device_id_type=MESH)
    pl.semaphore_wait(barrier, 3)
    wy(0).start()
    wy(1).start()

    gain = gain_ref[...].astype(F32)
    gain_f[...] = jnp.concatenate([gain[i:i + 1, :] for i in range(gain.shape[0])], axis=1)

    def trig(c, carry):
        cols = at(c, blk)
        angle = freq_ref[...] * pos_ref[:, cols].astype(F32)
        turns = jnp.floor(angle * (0.5 / math.pi) + 0.5)
        angle = ((angle - turns * 6.28125) - turns * 1.9350051879882812e-03) - turns * 3.0199159819e-07
        cosine, sine = jnp.cos(angle), jnp.sin(angle)
        cos_t[:, cols] = cosine
        sin_t[:, cols] = sine
        full = (at(c % 2, blk), at(c // 2, HEAD_DIM))
        s_even[full] = jnp.concatenate([cosine, cosine], axis=0).T
        s_odd[full] = jnp.concatenate([-sine, sine], axis=0).T
        return carry

    lax.fori_loop(0, n_blk, trig, 0)

    k_in.wait()

    def norm_k(r, carry):
        x_in(r).wait()
        rws = at(r, blk)

        def norm(i, inner):
            part = pl.ds(pl.multiple_of(r * blk + i * 32, 32), 32)
            x = y_ref[part, :].astype(F32)
            normed = x * lax.rsqrt(jnp.mean(x * x, axis=-1, keepdims=True) + NORM_EPS)
            hbuf[part, :] = (normed * gain_f[...]).astype(BF16)
            return inner

        lax.fori_loop(0, blk // 32, norm, 0)
        k = jnp.dot(hbuf[rws, :], wbuf[0], preferred_element_type=F32).astype(BF16)
        full = (at(r % 2, blk), at(r // 2, HEAD_DIM))
        for n in range(heads):
            vec = k[:, n * HEAD_DIM:(n + 1) * HEAD_DIM].astype(F32)
            rot = (vec * s_even[full] + pltpu.roll(vec, half, 1) * s_odd[full]).astype(BF16)
            kst_ref[rws, n * HEAD_DIM:(n + 1) * HEAD_DIM] = rot
            kv_ref[0, n, 0, rws, :] = rot
        return carry

    lax.fori_loop(0, n_blk, norm_k, 0)
    q_in(0).start()
    v_in.wait()

    def proj_v(r, carry):
        rws = at(r, blk)
        v = jnp.dot(hbuf[rws, :], wbuf[1], preferred_element_type=F32).astype(BF16)
        vst_ref[rws, :] = v
        for n in range(heads):
            for b in range(blk // HEAD_DIM):
                square = v[b * HEAD_DIM:(b + 1) * HEAD_DIM, n * HEAD_DIM:(n + 1) * HEAD_DIM].astype(F32).T.astype(BF16)
                kv_ref[0, n, 1, pl.ds(pl.multiple_of(r * blk + b * HEAD_DIM, HEAD_DIM), HEAD_DIM), :] = square
        return carry

    lax.fori_loop(0, n_blk, proj_v, 0)
    q_in(1).start()

    def proj_q(g, carry):
        q_in(g).wait()

        def rows_q(r, inner):
            rws = at(r, blk)
            q = jnp.dot(hbuf[rws, :], wbuf[g % 2], preferred_element_type=F32).astype(BF16)
            for n in range(heads):
                vec = q[:, n * HEAD_DIM:(n + 1) * HEAD_DIM].astype(F32).T
                a, b = vec[:half], vec[half:]
                out = jnp.concatenate([a * cos_t[:, rws] - b * sin_t[:, rws], b * cos_t[:, rws] + a * sin_t[:, rws]], axis=0)
                qt_ref[pl.ds(pl.multiple_of(g * width + n * HEAD_DIM, HEAD_DIM), HEAD_DIM), rws] = out.astype(BF16)

            @pl.when(jnp.logical_and(g == 0, r == 0))
            def _():
                kc().start()
                kx(0).start()
            return inner

        lax.fori_loop(0, n_blk, rows_q, 0)

        @pl.when(g < n_grp - 2)
        def _():
            q_in(g + 2).start()

        @pl.when(g == 1)
        def _():
            kx(1).start()
        return carry

    lax.fori_loop(0, n_grp, proj_q, 0)
    kx(2).start()
    pl.semaphore_signal(free_sem, inc=1, device_id=peer_y, device_id_type=MESH)
    for j in range(4):
        o_in(j).start()
    kc().wait()

    def attention(g, outer):
        kx(g).wait_recv()
        kd(g).start()

        @pl.when(g == 1)
        def _():
            kx(3).start()

        m_ref[...] = jnp.full_like(m_ref, -1e30)
        l_ref[...] = jnp.zeros_like(l_ref)
        att_ref[...] = jnp.zeros_like(att_ref)

        def scores(q_half, src, k_half, n, slot, diagonal):
            k = kv_ref[src, g, 0, at(k_half, seg), :]
            q = qt_ref[pl.ds(pl.multiple_of(g * width + n * HEAD_DIM, HEAD_DIM), HEAD_DIM), at(q_half, seg)]
            s = jnp.dot(k, q, preferred_element_type=F32)
            if diagonal:
                keep = lax.broadcasted_iota(jnp.int32, (seg, seg), 0) <= lax.broadcasted_iota(jnp.int32, (seg, seg), 1)
                s = jnp.where(keep, s, -1e30)
            s_refs[slot][...] = s
            return jnp.max(s.reshape(seg // 8, 8, seg), axis=0)

        def soften(q_half, n, slot, top):
            chunk = 64
            m_old = m_ref[q_half, n:n + 1, :]
            m_new = jnp.maximum(m_old, jnp.max(top, axis=0, keepdims=True))
            alpha = jnp.exp2((m_old - m_new) * SCALE_LOG2)
            shift = jnp.broadcast_to(m_new * SCALE_LOG2, (8, seg))
            m_ref[q_half, n:n + 1, :] = m_new
            total = jnp.zeros((8, seg), F32)
            for c in range(0, seg, chunk):
                s = s_refs[slot][c:c + chunk, :].reshape(chunk // 8, 8, seg)
                p = jnp.exp2(s * SCALE_LOG2 - shift[None])
                total = total + jnp.sum(p, axis=0)
                p_refs[slot][c:c + chunk, :] = p.reshape(chunk, seg).astype(BF16)
            l_ref[q_half, n:n + 1, :] = l_ref[q_half, n:n + 1, :] * alpha + jnp.sum(total, axis=0, keepdims=True)
            return alpha

        def weigh(q_half, src, k_half, n, slot, alpha):
            v_t = jnp.concatenate([kv_ref[src, g, 1, pl.ds(pl.multiple_of(k_half * seg + b, HEAD_DIM), HEAD_DIM), :]
                                   for b in range(0, seg, HEAD_DIM)], axis=1)
            rws = slice(n * HEAD_DIM, (n + 1) * HEAD_DIM)
            att_ref[q_half, rws, :] = att_ref[q_half, rws, :] * alpha + jnp.dot(
                v_t, p_refs[slot][...], preferred_element_type=F32)

        def block(q_half, src, k_half, top, following):
            previous = None
            for n in range(heads):
                if n + 1 < heads:
                    top_next = scores(q_half, src, k_half, n + 1, (n + 1) % 2, following is None)
                else:
                    top_next = None if following is None else scores(*following, 0, 0, False)
                alpha = soften(q_half, n, n % 2, top)
                if previous is not None:
                    weigh(*previous)
                previous = (q_half, src, k_half, n, n % 2, alpha)
                top = top_next
            weigh(*previous)
            return top

        def place(step):
            src = (step + 1) // 2
            near = 1 - src // 2
            lower = near * (me % 2) + (1 - near) * (me // 2)
            free = (1 - step % 2) * ((step + 6) // 7)
            return 1 - free * lower, src, free * (1 - lower)

        def on_diagonal(side, carry):
            block(side, 0, side, scores(side, 0, side, 0, 0, True), None)
            return carry

        lax.fori_loop(0, 2, on_diagonal, 0)
        kd(g).wait_recv()
        n_steps = 7

        def step_body(step, top):
            @pl.when(jnp.logical_and(g == 0, step == 5))
            def _():
                wy(2).start()
                wy(3).start()

            @pl.when(jnp.logical_and(g == 1, step == 2))
            def _():
                for w in (0, 1):
                    wy(w).wait_recv()
                    wx(w).start()
                    wc(w).start()

            @pl.when(jnp.logical_and(g == 3, step == 4))
            def _():
                pl.semaphore_wait(free_sem, 1)
                oy(0).start()
                oy(1).start()

            return block(*place(step), top, place(jnp.minimum(step + 1, n_steps - 1)))

        lax.fori_loop(0, n_steps, step_body, scores(*place(0), 0, 0, False))

        def write(q_half, carry):
            for n in range(heads):
                o = (att_ref[q_half, n * HEAD_DIM:(n + 1) * HEAD_DIM, :] / l_ref[q_half, n:n + 1, :]).T.astype(BF16)
                hbuf[at(q_half, seg), pl.ds(pl.multiple_of(g * width + n * HEAD_DIM, HEAD_DIM), HEAD_DIM)] = o
            return carry

        lax.fori_loop(0, 2, write, 0)
        return outer

    lax.fori_loop(0, n_grp, attention, 0)

    def out_own(j, carry):
        o_in(j).wait()

        def add(r, inner):
            acc_ref[at(r, blk), at(j, width)] = y_ref[at(r, blk), at(j, width)].astype(F32) + jnp.dot(
                hbuf[at(r, blk), 0:own_cols], o_tile(j)[...], preferred_element_type=F32)
            return inner

        lax.fori_loop(0, n_blk, add, 0)

        @pl.when(j < n_tile - 4)
        def _():
            o_in(j + 4).start()

        @pl.when(j == 1)
        def _():
            for w in (2, 3):
                wy(w).wait_recv()
                wx(w).start()
                wc(w).start()

        @pl.when(j == 5)
        def _():
            for w in (0, 1):
                wx(w).wait_recv()
                wd(w).start()

        @pl.when(j == 6)
        def _():
            oy(2).start()
        return carry

    lax.fori_loop(0, n_tile, out_own, 0)

    def load_group(g):
        wc(g).wait_recv()
        wd(g).wait_recv()
        for j in range(n_tile):
            w1_in(g, j).start()

    def add_group(g, r):
        def add(j, carry):
            acc_ref[at(r, blk), at(j, width)] += jnp.dot(
                hbuf[at(r, blk), at(g + n_grp, width)], wbuf[g % 2, at(j, width)], preferred_element_type=F32)
            return carry

        lax.fori_loop(0, n_tile, add, 0)

    def add_rows(g):
        def body(r, carry):
            add_group(g, r)
            return carry

        lax.fori_loop(0, n_blk, body, 0)

    load_group(0)
    load_group(1)
    oy(0).wait_recv()
    o_last(0).start()
    for j in range(n_tile):
        w1_in(0, j).wait()
    add_rows(0)
    oy(1).wait_recv()
    o_last(1).start()
    for w in (2, 3):
        wx(w).wait_recv()
        wd(w).start()
    for j in range(n_tile):
        w1_in(1, j).wait()
    add_rows(1)
    load_group(2)
    load_group(3)
    o_last(2).start()
    oy(2).wait_recv()
    for j in range(n_tile):
        w1_in(2, j).wait()
    add_rows(2)
    o_last(3).start()
    for j in range(n_tile):
        w1_in(3, j).wait()

    def finish(r, carry):
        o_last(r).wait_recv()
        add_group(n_grp - 1, r)


        def round_off(i, inner):
            part = pl.ds(pl.multiple_of(r * blk + i * 32, 32), 32)
            y_ref[part, :] = acc_ref[part, :].astype(BF16)
            return inner

        lax.fori_loop(0, blk // 32, round_off, 0)
        return carry

    lax.fori_loop(0, n_blk, finish, 0)

    for n in range(4):
        kx(n).wait_send()
        kd(n).wait_send()
        wy(n).wait_send()
        wx(n).wait_send()
        wc(n).wait_send()
        wd(n).wait_send()
        o_last(n).wait_send()
    for g in range(3):
        oy(g).wait_send()


def write_kernel(y_ref, k_ref, v_ref, y_hbm, k_hbm, v_hbm, k_buf, v_buf, sem):
    copies = [pltpu.make_async_copy(y_ref, y_hbm, sem.at[0]),
              pltpu.make_async_copy(k_buf, k_hbm, sem.at[1]),
              pltpu.make_async_copy(v_buf, v_hbm, sem.at[2])]
    copies[0].start()
    for n in range(k_buf.shape[1]):
        k_buf[:, n, :] = k_ref[:, n * HEAD_DIM:(n + 1) * HEAD_DIM]
    copies[1].start()
    for n in range(k_buf.shape[1]):
        v_buf[:, n, :] = v_ref[:, n * HEAD_DIM:(n + 1) * HEAD_DIM]
    copies[2].start()
    for copy in copies:
        copy.wait()


def solution(mesh):
    def device_fn(x_in, positions, norm_gain, w_q, w_k, w_v, w_o):
        rows, dim = x_in.shape
        cols = w_k.shape[1]
        kv_dev = cols // HEAD_DIM
        seg = rows // 2
        half = HEAD_DIM // 2
        hbm = pl.BlockSpec(memory_space=pl.ANY)
        vmem = pl.BlockSpec(memory_space=pltpu.VMEM)
        dma = pltpu.SemaphoreType.DMA
        y_raw, k_flat, v_flat, _ = pl.pallas_call(
            layer_kernel,
            in_specs=[hbm, vmem, vmem, vmem, hbm, hbm, hbm, hbm],
            out_specs=[vmem] * 3 + [hbm],
            out_shape=[
                pltpu.VMEM((rows, dim), BF16),
                pltpu.VMEM((rows, cols), BF16),
                pltpu.VMEM((rows, cols), BF16),
                jax.ShapeDtypeStruct(w_o.shape, BF16),
            ],
            scratch_shapes=[
                pltpu.VMEM((rows, dim), BF16),
                pltpu.VMEM((2, dim, cols), BF16),
                pltpu.VMEM((4, kv_dev, 2, rows, HEAD_DIM), BF16),
                pltpu.VMEM((w_q.shape[1], rows), BF16),
                pltpu.VMEM((seg, seg), F32),
                pltpu.VMEM((seg, seg), F32),
                pltpu.VMEM((seg, seg), BF16),
                pltpu.VMEM((seg, seg), BF16),
                pltpu.VMEM((2, 8, seg), F32),
                pltpu.VMEM((2, 8, seg), F32),
                pltpu.VMEM((2, cols, seg), F32),
                pltpu.VMEM((rows, dim), F32),
                pltpu.VMEM((half, rows), F32),
                pltpu.VMEM((half, rows), F32),
                pltpu.VMEM((1, dim), F32),
                dma((4,)), dma((4,)), dma((2, 8)),
                dma((4,)), dma((4,)), dma((4,)), dma((4,)), dma((4,)), dma((4,)), dma((4,)), dma((4,)),
                dma, dma, dma((4,)), dma((4,)), dma((4,)), dma((4,)),
                dma((3,)), dma((3,)), dma((4,)), dma((4,)),
                pltpu.SemaphoreType.REGULAR,
            ],
            compiler_params=pltpu.CompilerParams(collective_id=0, has_side_effects=True, vmem_limit_bytes=53 * 1024 * 1024),
            name="layer",
        )(x_in, positions.reshape(1, rows), jnp.asarray(rope_freqs())[:, None], norm_gain.reshape(dim // HEAD_DIM, HEAD_DIM), w_q, w_k, w_v, w_o)
        cache = jax.ShapeDtypeStruct((rows, kv_dev, HEAD_DIM), BF16)
        return pl.pallas_call(
            write_kernel,
            in_specs=[vmem] * 3,
            out_specs=[hbm] * 3,
            out_shape=[jax.ShapeDtypeStruct((rows, dim), BF16), cache, cache],
            scratch_shapes=[pltpu.VMEM(cache.shape, BF16), pltpu.VMEM(cache.shape, BF16), dma((3,))],
            compiler_params=pltpu.CompilerParams(vmem_limit_bytes=16 * 1024 * 1024),
            name="write",
        )(y_raw, k_flat, v_flat)

    row_spec = P(('dp', 'cp'), None)
    cache_spec = P(('dp', 'cp'), 'tp', None)
    return jax.shard_map(device_fn, mesh=mesh, in_specs=(row_spec, P(('dp', 'cp')), P(None), P(None, 'tp'), P(None, 'tp'), P(None, 'tp'), P('tp', None)), out_specs=(row_spec, cache_spec, cache_spec), check_vma=False)
```

```python
import math
import functools
import numpy as np
import jax
import jax.numpy as jnp
from jax import lax
from jax.experimental import pallas as pl
from jax.experimental.pallas import tpu as pltpu
from jax.sharding import PartitionSpec as P

HEAD_DIM = 128
NORM_EPS = 1e-5
SCALE_LOG2 = (1.0 / math.sqrt(HEAD_DIM)) * math.log2(math.e)
N_CP = 4
MESH = pl.DeviceIdType.MESH
BF16 = jnp.bfloat16
F32 = jnp.float32


def rope_freqs():
    exponent = np.arange(0, HEAD_DIM, 2) / HEAD_DIM
    base_freq = 1.0 / (500000.0 ** exponent)
    wave_len = 2.0 * math.pi / base_freq
    smooth = (8192.0 / wave_len - 1.0) / 3.0
    blended = (1.0 - smooth) * base_freq / 8.0 + smooth * base_freq
    freqs = np.where(wave_len < 2048.0, base_freq, np.where(wave_len > 8192.0, base_freq / 8.0, blended))
    return freqs.astype(np.float32)


def layer_kernel(x_hbm, pos_ref, freq_ref, gain_ref, wq_hbm, wk_hbm, wv_hbm, wo_hbm,
                 y_ref, kst_ref, vst_ref, w1_hbm,
                 hbuf, wbuf, kv_ref, qt_ref, s_even, s_odd, p_even, p_odd,
                 m_ref, l_ref, att_ref, acc_ref, cos_t, sin_t, gain_f,
                 x_sem, w_sem, f_sem,
                 wy_s, wy_r, wx_s, wx_r, wc_s, wc_r, wd_s, wd_r,
                 kc_s, kc_r, kx_s, kx_r, kd_s, kd_r, oy_s, oy_r, or_s, or_r, free_sem):
    rows, dim = hbuf.shape
    width = wk_hbm.shape[1]
    n_grp = wq_hbm.shape[1] // width
    own_cols = n_grp * width
    seg = rows // 2
    half = HEAD_DIM // 2
    blk = 256
    n_blk = rows // blk
    heads = width // HEAD_DIM
    me = lax.axis_index("cp")
    peer_y = {"tp": 1 - lax.axis_index("tp")}
    peer_c = {"cp": me + 1 - 2 * (me % 2)}
    peer_x = {"cp": (me + 2) % N_CP}
    s_refs, p_refs = (s_even, s_odd), (p_even, p_odd)

    def at(i, size):
        return pl.ds(pl.multiple_of(i * size, size), size)

    def remote(src, dst, send, recv, peer):
        return pltpu.make_async_remote_copy(src_ref=src, dst_ref=dst, send_sem=send, recv_sem=recv,
                                            device_id=peer, device_id_type=MESH)

    def w_rows(g, owner):
        return pl.ds(pl.multiple_of(g * width + owner * HEAD_DIM, HEAD_DIM), HEAD_DIM)

    other_x = (me + 2) % N_CP

    def wy(g):
        return remote(wo_hbm.at[w_rows(g, me)], w1_hbm.at[w_rows(g, me)], wy_s.at[g], wy_r.at[g], peer_y)

    def wx(g):
        return remote(w1_hbm.at[w_rows(g, me)], w1_hbm.at[w_rows(g, me)], wx_s.at[g], wx_r.at[g], peer_x)

    def wc(g):
        return remote(w1_hbm.at[w_rows(g, me)], w1_hbm.at[w_rows(g, me)], wc_s.at[g], wc_r.at[g], peer_c)

    def wd(g):
        return remote(w1_hbm.at[w_rows(g, other_x)], w1_hbm.at[w_rows(g, other_x)], wd_s.at[g], wd_r.at[g], peer_c)

    def kc():
        return remote(kv_ref.at[0], kv_ref.at[1], kc_s, kc_r, peer_c)

    def kx(n):
        return remote(kv_ref.at[0, n], kv_ref.at[2, n], kx_s.at[n], kx_r.at[n], peer_x)

    def kd(n):
        return remote(kv_ref.at[2, n], kv_ref.at[3, n], kd_s.at[n], kd_r.at[n], peer_c)

    def oy(g):
        return remote(hbuf.at[:, at(g, width)], hbuf.at[:, at(g + n_grp, width)], oy_s.at[g], oy_r.at[g], peer_y)

    def o_last(r):
        g = n_grp - 1
        return remote(hbuf.at[at(r, blk), at(g, width)], hbuf.at[at(r, blk), at(g + n_grp, width)],
                      or_s.at[r], or_r.at[r], peer_y)

    def x_in(r):
        return pltpu.make_async_copy(x_hbm.at[at(r, blk)], y_ref.at[at(r, blk)], x_sem.at[r])

    def q_in(g):
        return pltpu.make_async_copy(wq_hbm.at[:, at(g, width)], wbuf.at[g % 2], w_sem.at[g % 2])

    def o_tile(j):
        return wbuf.at[(j % 4) // 2, at(j % 2, own_cols)]

    def o_in(j):
        return pltpu.make_async_copy(wo_hbm.at[:, at(j, width)], o_tile(j), w_sem.at[j % 4])

    n_tile = dim // width

    def w1_in(g, j):
        return pltpu.make_async_copy(w1_hbm.at[at(g, width), at(j, width)], wbuf.at[g % 2, at(j, width)], f_sem.at[g % 2, j])

    k_in = pltpu.make_async_copy(wk_hbm, wbuf.at[0], w_sem.at[0])
    v_in = pltpu.make_async_copy(wv_hbm, wbuf.at[1], w_sem.at[1])

    def share(w):
        wy(w).wait_recv()
        wx(w).start()
        wc(w).start()

    def pass_on(w):
        wx(w).wait_recv()
        wd(w).start()

    def load_group(g):
        wc(g).wait_recv()
        wd(g).wait_recv()
        for j in range(n_tile):
            w1_in(g, j).start()

    x_in(0).start()
    k_in.start()
    x_in(1).start()
    v_in.start()
    x_in(2).start()
    x_in(3).start()
    barrier = pltpu.get_barrier_semaphore()
    for peer in (peer_y, peer_c, peer_x):
        pl.semaphore_signal(barrier, inc=1, device_id=peer, device_id_type=MESH)
    pl.semaphore_wait(barrier, 3)
    wy(0).start()

    gain = gain_ref[...].astype(F32)
    gain_f[...] = jnp.concatenate([gain[i:i + 1, :] for i in range(gain.shape[0])], axis=1)

    def trig(c, carry):
        cols = at(c, blk)
        angle = freq_ref[...] * pos_ref[:, cols].astype(F32)
        turns = jnp.floor(angle * (0.5 / math.pi) + 0.5)
        angle = ((angle - turns * 6.28125) - turns * 1.9350051879882812e-03) - turns * 3.0199159819e-07
        cosine, sine = jnp.cos(angle), jnp.sin(angle)
        cos_t[:, cols] = cosine
        sin_t[:, cols] = sine
        full = (at(c % 2, blk), at(c // 2, HEAD_DIM))
        s_even[full] = jnp.concatenate([cosine, cosine], axis=0).T
        s_odd[full] = jnp.concatenate([-sine, sine], axis=0).T
        return carry

    lax.fori_loop(0, n_blk, trig, 0)

    k_in.wait()

    def norm_k(r, carry):
        x_in(r).wait()
        rws = at(r, blk)

        def norm(i, inner):
            part = pl.ds(pl.multiple_of(r * blk + i * 32, 32), 32)
            x = y_ref[part, :].astype(F32)
            normed = x * lax.rsqrt(jnp.mean(x * x, axis=-1, keepdims=True) + NORM_EPS)
            hbuf[part, :] = (normed * gain_f[...]).astype(BF16)
            return inner

        lax.fori_loop(0, blk // 32, norm, 0)
        k = jnp.dot(hbuf[rws, :], wbuf[0], preferred_element_type=F32).astype(BF16)
        full = (at(r % 2, blk), at(r // 2, HEAD_DIM))
        for n in range(heads):
            vec = k[:, n * HEAD_DIM:(n + 1) * HEAD_DIM].astype(F32)
            rot = (vec * s_even[full] + pltpu.roll(vec, half, 1) * s_odd[full]).astype(BF16)
            kv_ref[0, n, 0, rws, :] = rot
        return carry

    lax.fori_loop(0, n_blk, norm_k, 0)
    q_in(0).start()
    v_in.wait()

    def proj_v(r, carry):
        rws = at(r, blk)
        v = jnp.dot(hbuf[rws, :], wbuf[1], preferred_element_type=F32).astype(BF16)
        for n in range(heads):
            for b in range(blk // HEAD_DIM):
                square = v[b * HEAD_DIM:(b + 1) * HEAD_DIM, n * HEAD_DIM:(n + 1) * HEAD_DIM].astype(F32).T.astype(BF16)
                kv_ref[0, n, 1, pl.ds(pl.multiple_of(r * blk + b * HEAD_DIM, HEAD_DIM), HEAD_DIM), :] = square

        @pl.when(r == n_blk - 2)
        def _():
            wy(1).start()
        return carry

    lax.fori_loop(0, n_blk, proj_v, 0)
    q_in(1).start()

    def proj_q(g, carry):
        q_in(g).wait()

        def rows_q(r, inner):
            rws = at(r, blk)
            q = jnp.dot(hbuf[rws, :], wbuf[g % 2], preferred_element_type=F32).astype(BF16)
            for n in range(heads):
                vec = q[:, n * HEAD_DIM:(n + 1) * HEAD_DIM].astype(F32).T
                a, b = vec[:half], vec[half:]
                out = jnp.concatenate([a * cos_t[:, rws] - b * sin_t[:, rws], b * cos_t[:, rws] + a * sin_t[:, rws]], axis=0)
                qt_ref[pl.ds(pl.multiple_of(g * width + n * HEAD_DIM, HEAD_DIM), HEAD_DIM), rws] = out.astype(BF16)

            @pl.when(jnp.logical_and(g == 0, r == 0))
            def _():
                kc().start()
                kx(0).start()

            @pl.when(jnp.logical_and(g == n_grp - 1, r == 2))
            def _():
                wy(2).start()
            return inner

        lax.fori_loop(0, n_blk, rows_q, 0)

        @pl.when(g < n_grp - 2)
        def _():
            q_in(g + 2).start()

        @pl.when(g == 1)
        def _():
            kx(1).start()
        return carry

    lax.fori_loop(0, n_grp, proj_q, 0)
    kx(2).start()
    pl.semaphore_signal(free_sem, inc=1, device_id=peer_y, device_id_type=MESH)
    for j in range(4):
        o_in(j).start()
    kc().wait()

    def attention(g, outer):
        kx(g).wait_recv()
        kd(g).start()

        m_ref[...] = jnp.full_like(m_ref, -1e30)
        l_ref[...] = jnp.zeros_like(l_ref)
        att_ref[...] = jnp.zeros_like(att_ref)

        def scores(q_half, src, k_half, n, slot, diagonal):
            k = kv_ref[src, g, 0, at(k_half, seg), :]
            q = qt_ref[pl.ds(pl.multiple_of(g * width + n * HEAD_DIM, HEAD_DIM), HEAD_DIM), at(q_half, seg)]
            s = jnp.dot(k, q, preferred_element_type=F32)
            if diagonal:
                keep = lax.broadcasted_iota(jnp.int32, (seg, seg), 0) <= lax.broadcasted_iota(jnp.int32, (seg, seg), 1)
                s = jnp.where(keep, s, -1e30)
            s_refs[slot][...] = s
            return jnp.max(s.reshape(seg // 8, 8, seg), axis=0)

        def soften(q_half, n, slot, top):
            chunk = 64
            m_old = m_ref[q_half, n:n + 1, :]
            m_new = jnp.maximum(m_old, jnp.max(top, axis=0, keepdims=True))
            alpha = jnp.exp2((m_old - m_new) * SCALE_LOG2)
            shift = jnp.broadcast_to(m_new * SCALE_LOG2, (8, seg))
            m_ref[q_half, n:n + 1, :] = m_new
            total = jnp.zeros((8, seg), F32)
            for c in range(0, seg, chunk):
                s = s_refs[slot][c:c + chunk, :].reshape(chunk // 8, 8, seg)
                p = jnp.exp2(s * SCALE_LOG2 - shift[None])
                total = total + jnp.sum(p, axis=0)
                p_refs[slot][c:c + chunk, :] = p.reshape(chunk, seg).astype(BF16)
            l_ref[q_half, n:n + 1, :] = l_ref[q_half, n:n + 1, :] * alpha + jnp.sum(total, axis=0, keepdims=True)
            return alpha

        def weigh(q_half, src, k_half, n, slot, alpha):
            v_t = jnp.concatenate([kv_ref[src, g, 1, pl.ds(pl.multiple_of(k_half * seg + b, HEAD_DIM), HEAD_DIM), :]
                                   for b in range(0, seg, HEAD_DIM)], axis=1)
            rws = slice(n * HEAD_DIM, (n + 1) * HEAD_DIM)
            att_ref[q_half, rws, :] = att_ref[q_half, rws, :] * alpha + jnp.dot(
                v_t, p_refs[slot][...], preferred_element_type=F32)

        def block(q_half, src, k_half, top, following):
            previous = None
            for n in range(heads):
                if n + 1 < heads:
                    top_next = scores(q_half, src, k_half, n + 1, (n + 1) % 2, following is None)
                else:
                    top_next = None if following is None else scores(*following, 0, 0, False)
                alpha = soften(q_half, n, n % 2, top)
                if previous is not None:
                    weigh(*previous)
                previous = (q_half, src, k_half, n, n % 2, alpha)
                top = top_next
            weigh(*previous)
            return top

        def place(step):
            src = (step + 1) // 2
            near = 1 - src // 2
            lower = near * (me % 2) + (1 - near) * (me // 2)
            free = (1 - step % 2) * ((step + 6) // 7)
            return 1 - free * lower, src, free * (1 - lower)

        def on_diagonal(side, carry):
            block(side, 0, side, scores(side, 0, side, 0, 0, True), None)
            return carry

        lax.fori_loop(0, 2, on_diagonal, 0)
        kd(g).wait_recv()
        n_steps = 7

        def step_body(step, top):
            @pl.when(jnp.logical_and(g == 0, step == 6))
            def _():
                share(0)

            @pl.when(jnp.logical_and(g == 1, step == 2))
            def _():
                wy(3).start()

            @pl.when(jnp.logical_and(g == 1, step == 3))
            def _():
                kx(3).start()

            @pl.when(jnp.logical_and(g == 2, step == 6))
            def _():
                pl.semaphore_wait(free_sem, 1)
                oy(0).start()
                share(1)

            return block(*place(step), top, place(jnp.minimum(step + 1, n_steps - 1)))

        lax.fori_loop(0, n_steps, step_body, scores(*place(0), 0, 0, False))

        def write(q_half, carry):
            for n in range(heads):
                o = (att_ref[q_half, n * HEAD_DIM:(n + 1) * HEAD_DIM, :] / l_ref[q_half, n:n + 1, :]).T.astype(BF16)
                hbuf[at(q_half, seg), pl.ds(pl.multiple_of(g * width + n * HEAD_DIM, HEAD_DIM), HEAD_DIM)] = o
            return carry

        lax.fori_loop(0, 2, write, 0)
        return outer

    lax.fori_loop(0, n_grp, attention, 0)

    def out_own(j, carry):
        o_in(j).wait()
        cols = at(j, width)
        for r in range(n_blk):
            rws = slice(r * blk, (r + 1) * blk)
            acc_ref[rws, cols] = y_ref[rws, cols].astype(F32) + jnp.dot(
                hbuf[rws, 0:own_cols], o_tile(j)[...], preferred_element_type=F32)

        @pl.when(j < n_tile - 4)
        def _():
            o_in(j + 4).start()

        @pl.when(j == 0)
        def _():
            pass_on(0)

        @pl.when(j == 1)
        def _():
            oy(1).start()
            share(2)

        @pl.when(j == 5)
        def _():
            pass_on(1)
            load_group(0)
        return carry

    lax.fori_loop(0, n_tile, out_own, 0)

    def add_group(g, tick=None):
        for j in range(n_tile):
            w1_in(g, j).wait()

        def add(j, carry):
            for r in range(n_blk):
                rws = slice(r * blk, (r + 1) * blk)
                acc_ref[rws, at(j, width)] += jnp.dot(
                    hbuf[rws, at(g + n_grp, width)], wbuf[g % 2, at(j, width)], preferred_element_type=F32)
            if tick is not None:
                pl.when(j == n_tile // 2)(tick)
            return carry

        lax.fori_loop(0, n_tile, add, 0)

    load_group(1)
    oy(0).wait_recv()
    add_group(0, lambda: oy(2).start())
    share(3)
    oy(1).wait_recv()
    add_group(1)
    pass_on(2)
    o_last(0).start()

    def caches(c, carry):
        rws = at(c, HEAD_DIM)
        for n in range(heads):
            kst_ref[rws, n, :] = kv_ref[0, n, 0, rws, :]
            vst_ref[rws, n, :] = kv_ref[0, n, 1, rws, :].astype(F32).T.astype(BF16)
        return carry

    lax.fori_loop(0, rows // HEAD_DIM, caches, 0)
    load_group(2)
    o_last(0).wait_recv()
    o_last(1).start()
    pass_on(3)
    oy(2).wait_recv()
    o_last(2).start()
    load_group(3)
    add_group(2, lambda: o_last(3).start())
    for j in range(n_tile):
        w1_in(3, j).wait()

    def finish(r, carry):
        @pl.when(r > 0)
        def _():
            o_last(r).wait_recv()

        rws = at(r, blk)
        for j in range(n_tile):
            cols = slice(j * width, (j + 1) * width)
            total = acc_ref[rws, cols] + jnp.dot(hbuf[rws, at(2 * n_grp - 1, width)], wbuf[1, at(j, width)],
                                                 preferred_element_type=F32)
            y_ref[rws, cols] = total.astype(BF16)
        return carry

    lax.fori_loop(0, n_blk, finish, 0)

    for n in range(4):
        kx(n).wait_send()
        kd(n).wait_send()
        wy(n).wait_send()
        wx(n).wait_send()
        wc(n).wait_send()
        wd(n).wait_send()
        o_last(n).wait_send()
    for g in range(3):
        oy(g).wait_send()


def write_kernel(y_ref, k_ref, v_ref, y_hbm, k_hbm, v_hbm, sem):
    pieces = 8
    size = y_ref.shape[0] // pieces
    copies = []
    for i in range(pieces):
        part = pl.ds(i * size, size)
        copies.append(pltpu.make_async_copy(y_ref.at[part], y_hbm.at[part], sem.at[i]))
    copies.append(pltpu.make_async_copy(k_ref, k_hbm, sem.at[pieces]))
    copies.append(pltpu.make_async_copy(v_ref, v_hbm, sem.at[pieces + 1]))
    for copy in copies:
        copy.start()
    for copy in copies:
        copy.wait()


def solution(mesh):
    def device_fn(x_in, positions, norm_gain, w_q, w_k, w_v, w_o):
        rows, dim = x_in.shape
        cols = w_k.shape[1]
        kv_dev = cols // HEAD_DIM
        seg = rows // 2
        half = HEAD_DIM // 2
        hbm = pl.BlockSpec(memory_space=pl.ANY)
        vmem = pl.BlockSpec(memory_space=pltpu.VMEM)
        dma = pltpu.SemaphoreType.DMA
        y_raw, k_flat, v_flat, _ = pl.pallas_call(
            layer_kernel,
            in_specs=[hbm, vmem, vmem, vmem, hbm, hbm, hbm, hbm],
            out_specs=[vmem] * 3 + [hbm],
            out_shape=[
                pltpu.VMEM((rows, dim), BF16),
                pltpu.VMEM((rows, kv_dev, HEAD_DIM), BF16),
                pltpu.VMEM((rows, kv_dev, HEAD_DIM), BF16),
                jax.ShapeDtypeStruct(w_o.shape, BF16),
            ],
            scratch_shapes=[
                pltpu.VMEM((rows, dim), BF16),
                pltpu.VMEM((2, dim, cols), BF16),
                pltpu.VMEM((4, kv_dev, 2, rows, HEAD_DIM), BF16),
                pltpu.VMEM((w_q.shape[1], rows), BF16),
                pltpu.VMEM((seg, seg), F32),
                pltpu.VMEM((seg, seg), F32),
                pltpu.VMEM((seg, seg), BF16),
                pltpu.VMEM((seg, seg), BF16),
                pltpu.VMEM((2, 8, seg), F32),
                pltpu.VMEM((2, 8, seg), F32),
                pltpu.VMEM((2, cols, seg), F32),
                pltpu.VMEM((rows, dim), F32),
                pltpu.VMEM((half, rows), F32),
                pltpu.VMEM((half, rows), F32),
                pltpu.VMEM((1, dim), F32),
                dma((4,)), dma((4,)), dma((2, 8)),
                dma((4,)), dma((4,)), dma((4,)), dma((4,)), dma((4,)), dma((4,)), dma((4,)), dma((4,)),
                dma, dma, dma((4,)), dma((4,)), dma((4,)), dma((4,)),
                dma((3,)), dma((3,)), dma((4,)), dma((4,)),
                pltpu.SemaphoreType.REGULAR,
            ],
            compiler_params=pltpu.CompilerParams(collective_id=0, has_side_effects=True, vmem_limit_bytes=53 * 1024 * 1024),
            name="layer",
        )(x_in, positions.reshape(1, rows), jnp.asarray(rope_freqs())[:, None], norm_gain.reshape(dim // HEAD_DIM, HEAD_DIM), w_q, w_k, w_v, w_o)
        cache = jax.ShapeDtypeStruct((rows, kv_dev, HEAD_DIM), BF16)
        return pl.pallas_call(
            write_kernel,
            in_specs=[vmem] * 3,
            out_specs=[hbm] * 3,
            out_shape=[jax.ShapeDtypeStruct((rows, dim), BF16), cache, cache],
            scratch_shapes=[dma((10,))],
            compiler_params=pltpu.CompilerParams(vmem_limit_bytes=2 * 1024 * 1024),
            name="write",
        )(y_raw, k_flat, v_flat)

    row_spec = P(('dp', 'cp'), None)
    cache_spec = P(('dp', 'cp'), 'tp', None)
    return jax.shard_map(device_fn, mesh=mesh, in_specs=(row_spec, P(('dp', 'cp')), P(None), P(None, 'tp'), P(None, 'tp'), P(None, 'tp'), P('tp', None)), out_specs=(row_spec, cache_spec, cache_spec), check_vma=False)
```

```python
import math
import functools
import numpy as np
import jax
import jax.numpy as jnp
from jax import lax
from jax.experimental import pallas as pl
from jax.experimental.pallas import tpu as pltpu
from jax.sharding import PartitionSpec as P

HEAD_DIM = 128
NORM_EPS = 1e-5
SCALE_LOG2 = (1.0 / math.sqrt(HEAD_DIM)) * math.log2(math.e)
N_CP = 4
MESH = pl.DeviceIdType.MESH
BF16 = jnp.bfloat16
F32 = jnp.float32


def rope_freqs():
    exponent = np.arange(0, HEAD_DIM, 2) / HEAD_DIM
    base_freq = 1.0 / (500000.0 ** exponent)
    wave_len = 2.0 * math.pi / base_freq
    smooth = (8192.0 / wave_len - 1.0) / 3.0
    blended = (1.0 - smooth) * base_freq / 8.0 + smooth * base_freq
    freqs = np.where(wave_len < 2048.0, base_freq, np.where(wave_len > 8192.0, base_freq / 8.0, blended))
    return freqs.astype(np.float32)


def layer_kernel(x_hbm, pos_hbm, freq_hbm, gain_hbm, wq_hbm, wk_hbm, wv_hbm, wo_hbm,
                 y_ref, kst_ref, vst_ref, w1_hbm,
                 hbuf, wbuf, kv_ref, qt_ref, s_even, s_odd, p_even, p_odd,
                 m_ref, l_ref, att_ref, acc_ref, cos_t, sin_t, gain_f, pos_ref, freq_ref, gain_ref,
                 x_sem, w_sem, f_sem, t_sem,
                 wy_s, wy_r, wx_s, wx_r, wc_s, wc_r, wd_s, wd_r,
                 kc_s, kc_r, kx_s, kx_r, kd_s, kd_r, oy_s, oy_r, or_s, or_r, free_sem):
    rows, dim = hbuf.shape
    width = wk_hbm.shape[1]
    n_grp = wq_hbm.shape[1] // width
    own_cols = n_grp * width
    seg = rows // 2
    half = HEAD_DIM // 2
    blk = 256
    n_blk = rows // blk
    heads = width // HEAD_DIM
    me = lax.axis_index("cp")
    peer_y = {"tp": 1 - lax.axis_index("tp")}
    peer_c = {"cp": me + 1 - 2 * (me % 2)}
    peer_x = {"cp": (me + 2) % N_CP}
    s_refs, p_refs = (s_even, s_odd), (p_even, p_odd)

    def at(i, size):
        return pl.ds(pl.multiple_of(i * size, size), size)

    def remote(src, dst, send, recv, peer):
        return pltpu.make_async_remote_copy(src_ref=src, dst_ref=dst, send_sem=send, recv_sem=recv,
                                            device_id=peer, device_id_type=MESH)

    def w_rows(g, owner):
        return pl.ds(pl.multiple_of(g * width + owner * HEAD_DIM, HEAD_DIM), HEAD_DIM)

    other_x = (me + 2) % N_CP

    def wy(g):
        return remote(wo_hbm.at[w_rows(g, me)], w1_hbm.at[w_rows(g, me)], wy_s.at[g], wy_r.at[g], peer_y)

    def wx(g):
        return remote(w1_hbm.at[w_rows(g, me)], w1_hbm.at[w_rows(g, me)], wx_s.at[g], wx_r.at[g], peer_x)

    def wc(g):
        return remote(w1_hbm.at[w_rows(g, me)], w1_hbm.at[w_rows(g, me)], wc_s.at[g], wc_r.at[g], peer_c)

    def wd(g):
        return remote(w1_hbm.at[w_rows(g, other_x)], w1_hbm.at[w_rows(g, other_x)], wd_s.at[g], wd_r.at[g], peer_c)

    def kc():
        return remote(kv_ref.at[0], kv_ref.at[1], kc_s, kc_r, peer_c)

    def kx(n):
        return remote(kv_ref.at[0, n], kv_ref.at[2, n], kx_s.at[n], kx_r.at[n], peer_x)

    def kd(n):
        return remote(kv_ref.at[2, n], kv_ref.at[3, n], kd_s.at[n], kd_r.at[n], peer_c)

    def oy(g):
        return remote(hbuf.at[:, at(g, width)], hbuf.at[:, at(g + n_grp, width)], oy_s.at[g], oy_r.at[g], peer_y)

    tail_rows = (256, 256, 256, 128, 128)
    tail = [pl.ds(sum(tail_rows[:r]), tail_rows[r]) for r in range(len(tail_rows))]

    def o_last(r):
        g = n_grp - 1
        return remote(hbuf.at[tail[r], at(g, width)], hbuf.at[tail[r], at(g + n_grp, width)],
                      or_s.at[r], or_r.at[r], peer_y)

    def x_in(r):
        return pltpu.make_async_copy(x_hbm.at[at(r, blk)], y_ref.at[at(r, blk)], x_sem.at[r])

    def q_in(g):
        return pltpu.make_async_copy(wq_hbm.at[:, at(g, width)], wbuf.at[g % 2], w_sem.at[g % 2])

    def o_tile(j):
        return wbuf.at[(j % 4) // 2, at(j % 2, own_cols)]

    def o_in(j):
        return pltpu.make_async_copy(wo_hbm.at[:, at(j, width)], o_tile(j), w_sem.at[j % 4])

    n_tile = dim // width

    def w1_in(g, j):
        return pltpu.make_async_copy(w1_hbm.at[at(g, width), at(j, width)], wbuf.at[g % 2, at(j, width)], f_sem.at[g % 2, j])

    k_in = pltpu.make_async_copy(wk_hbm, wbuf.at[0], w_sem.at[0])
    v_in = pltpu.make_async_copy(wv_hbm, wbuf.at[1], w_sem.at[1])

    def share(w):
        wy(w).wait_recv()
        wx(w).start()
        wc(w).start()

    def pass_on(w):
        wx(w).wait_recv()
        wd(w).start()

    def load_group(g):
        wc(g).wait_recv()
        wd(g).wait_recv()
        for j in range(n_tile):
            w1_in(g, j).start()

    barrier = pltpu.get_barrier_semaphore()
    for peer in (peer_y, peer_c, peer_x):
        pl.semaphore_signal(barrier, inc=1, device_id=peer, device_id_type=MESH)
    tables = [pltpu.make_async_copy(src, dst, t_sem.at[n])
              for n, (src, dst) in enumerate(((pos_hbm, pos_ref), (freq_hbm, freq_ref), (gain_hbm, gain_ref)))]
    for copy in tables:
        copy.start()
    x_in(0).start()
    k_in.start()
    x_in(1).start()
    v_in.start()
    x_in(2).start()
    x_in(3).start()
    pl.semaphore_wait(barrier, 3)
    wy(0).start()
    for copy in tables:
        copy.wait()
    gain = gain_ref[...].astype(F32)
    gain_f[...] = jnp.concatenate([gain[i:i + 1, :] for i in range(gain.shape[0])], axis=1)

    def trig(c, carry):
        cols = at(c, blk)
        angle = freq_ref[...] * pos_ref[:, cols].astype(F32)
        turns = jnp.floor(angle * (0.5 / math.pi) + 0.5)
        angle = ((angle - turns * 6.28125) - turns * 1.9350051879882812e-03) - turns * 3.0199159819e-07
        cosine, sine = jnp.cos(angle), jnp.sin(angle)
        cos_t[:, cols] = cosine
        sin_t[:, cols] = sine
        full = (at(c % 2, blk), at(c // 2, HEAD_DIM))
        s_even[full] = jnp.concatenate([cosine, cosine], axis=0).T
        s_odd[full] = jnp.concatenate([-sine, sine], axis=0).T
        return carry

    lax.fori_loop(0, n_blk, trig, 0)

    k_in.wait()

    def norm_k(r, carry):
        x_in(r).wait()
        rws = at(r, blk)

        def norm(i, inner):
            part = pl.ds(pl.multiple_of(r * blk + i * 32, 32), 32)
            x = y_ref[part, :].astype(F32)
            normed = x * lax.rsqrt(jnp.mean(x * x, axis=-1, keepdims=True) + NORM_EPS)
            hbuf[part, :] = (normed * gain_f[...]).astype(BF16)
            return inner

        lax.fori_loop(0, blk // 32, norm, 0)
        k = jnp.dot(hbuf[rws, :], wbuf[0], preferred_element_type=F32).astype(BF16)
        full = (at(r % 2, blk), at(r // 2, HEAD_DIM))
        for n in range(heads):
            vec = k[:, n * HEAD_DIM:(n + 1) * HEAD_DIM].astype(F32)
            rot = (vec * s_even[full] + pltpu.roll(vec, half, 1) * s_odd[full]).astype(BF16)
            kv_ref[0, n, 0, rws, :] = rot
        return carry

    lax.fori_loop(0, n_blk, norm_k, 0)
    q_in(0).start()
    v_in.wait()

    def proj_v(r, carry):
        rws = at(r, blk)
        v = jnp.dot(hbuf[rws, :], wbuf[1], preferred_element_type=F32).astype(BF16)
        for n in range(heads):
            for b in range(blk // HEAD_DIM):
                square = v[b * HEAD_DIM:(b + 1) * HEAD_DIM, n * HEAD_DIM:(n + 1) * HEAD_DIM].astype(F32).T.astype(BF16)
                kv_ref[0, n, 1, pl.ds(pl.multiple_of(r * blk + b * HEAD_DIM, HEAD_DIM), HEAD_DIM), :] = square

        @pl.when(r == n_blk - 2)
        def _():
            wy(1).start()
        return carry

    lax.fori_loop(0, n_blk, proj_v, 0)
    q_in(1).start()

    def proj_q(g, carry):
        q_in(g).wait()

        def rows_q(r, inner):
            rws = at(r, blk)
            q = jnp.dot(hbuf[rws, :], wbuf[g % 2], preferred_element_type=F32).astype(BF16)
            for n in range(heads):
                vec = q[:, n * HEAD_DIM:(n + 1) * HEAD_DIM].astype(F32).T
                a, b = vec[:half], vec[half:]
                out = jnp.concatenate([a * cos_t[:, rws] - b * sin_t[:, rws], b * cos_t[:, rws] + a * sin_t[:, rws]], axis=0)
                qt_ref[pl.ds(pl.multiple_of(g * width + n * HEAD_DIM, HEAD_DIM), HEAD_DIM), rws] = out.astype(BF16)

            @pl.when(jnp.logical_and(g == 0, r == 0))
            def _():
                kc().start()
                kx(0).start()

            @pl.when(jnp.logical_and(g == n_grp - 1, r == 2))
            def _():
                wy(2).start()
            return inner

        lax.fori_loop(0, n_blk, rows_q, 0)

        @pl.when(g < n_grp - 2)
        def _():
            q_in(g + 2).start()

        @pl.when(g == 1)
        def _():
            kx(1).start()
        return carry

    lax.fori_loop(0, n_grp, proj_q, 0)
    kx(2).start()
    pl.semaphore_signal(free_sem, inc=1, device_id=peer_y, device_id_type=MESH)
    for j in range(4):
        o_in(j).start()
    kc().wait()

    def attention(g, outer):
        kx(g).wait_recv()
        kd(g).start()

        m_ref[...] = jnp.full_like(m_ref, -1e30)
        l_ref[...] = jnp.zeros_like(l_ref)
        att_ref[...] = jnp.zeros_like(att_ref)

        def scores(q_half, src, k_half, n, slot, diagonal):
            k = kv_ref[src, g, 0, at(k_half, seg), :]
            q = qt_ref[pl.ds(pl.multiple_of(g * width + n * HEAD_DIM, HEAD_DIM), HEAD_DIM), at(q_half, seg)]
            s = jnp.dot(k, q, preferred_element_type=F32)
            if diagonal:
                keep = lax.broadcasted_iota(jnp.int32, (seg, seg), 0) <= lax.broadcasted_iota(jnp.int32, (seg, seg), 1)
                s = jnp.where(keep, s, -1e30)
            s_refs[slot][...] = s
            return jnp.max(s.reshape(seg // 8, 8, seg), axis=0)

        def soften(q_half, n, slot, top):
            chunk = 64
            m_old = m_ref[q_half, n:n + 1, :]
            m_new = jnp.maximum(m_old, jnp.max(top, axis=0, keepdims=True))
            alpha = jnp.exp2((m_old - m_new) * SCALE_LOG2)
            shift = jnp.broadcast_to(m_new * SCALE_LOG2, (8, seg))
            m_ref[q_half, n:n + 1, :] = m_new
            total = jnp.zeros((8, seg), F32)
            for c in range(0, seg, chunk):
                s = s_refs[slot][c:c + chunk, :].reshape(chunk // 8, 8, seg)
                p = jnp.exp2(s * SCALE_LOG2 - shift[None])
                total = total + jnp.sum(p, axis=0)
                p_refs[slot][c:c + chunk, :] = p.reshape(chunk, seg).astype(BF16)
            l_ref[q_half, n:n + 1, :] = l_ref[q_half, n:n + 1, :] * alpha + jnp.sum(total, axis=0, keepdims=True)
            return alpha

        def weigh(q_half, src, k_half, n, slot, alpha):
            v_t = jnp.concatenate([kv_ref[src, g, 1, pl.ds(pl.multiple_of(k_half * seg + b, HEAD_DIM), HEAD_DIM), :]
                                   for b in range(0, seg, HEAD_DIM)], axis=1)
            rws = slice(n * HEAD_DIM, (n + 1) * HEAD_DIM)
            att_ref[q_half, rws, :] = att_ref[q_half, rws, :] * alpha + jnp.dot(
                v_t, p_refs[slot][...], preferred_element_type=F32)

        def block(q_half, src, k_half, top, following):
            previous = None
            for n in range(heads):
                if n + 1 < heads:
                    top_next = scores(q_half, src, k_half, n + 1, (n + 1) % 2, following is None)
                else:
                    top_next = None if following is None else scores(*following, 0, 0, False)
                alpha = soften(q_half, n, n % 2, top)
                if previous is not None:
                    weigh(*previous)
                previous = (q_half, src, k_half, n, n % 2, alpha)
                top = top_next
            weigh(*previous)
            return top

        def place(step):
            src = (step + 1) // 2
            near = 1 - src // 2
            lower = near * (me % 2) + (1 - near) * (me // 2)
            free = (1 - step % 2) * ((step + 6) // 7)
            return 1 - free * lower, src, free * (1 - lower)

        def on_diagonal(side, carry):
            block(side, 0, side, scores(side, 0, side, 0, 0, True), None)
            return carry

        lax.fori_loop(0, 2, on_diagonal, 0)
        kd(g).wait_recv()
        n_steps = 7

        def step_body(step, top):
            @pl.when(jnp.logical_and(g == 0, step == 6))
            def _():
                share(0)

            @pl.when(jnp.logical_and(g == 1, step == 2))
            def _():
                wy(3).start()

            @pl.when(jnp.logical_and(g == 1, step == 3))
            def _():
                kx(3).start()

            @pl.when(jnp.logical_and(g == 2, step == 6))
            def _():
                pl.semaphore_wait(free_sem, 1)
                oy(0).start()
                share(1)

            return block(*place(step), top, place(jnp.minimum(step + 1, n_steps - 1)))

        lax.fori_loop(0, n_steps, step_body, scores(*place(0), 0, 0, False))

        def write(q_half, carry):
            for n in range(heads):
                o = (att_ref[q_half, n * HEAD_DIM:(n + 1) * HEAD_DIM, :] / l_ref[q_half, n:n + 1, :]).T.astype(BF16)
                hbuf[at(q_half, seg), pl.ds(pl.multiple_of(g * width + n * HEAD_DIM, HEAD_DIM), HEAD_DIM)] = o
            return carry

        lax.fori_loop(0, 2, write, 0)
        return outer

    lax.fori_loop(0, n_grp, attention, 0)

    def out_own(j, carry):
        o_in(j).wait()
        cols = at(j, width)
        for r in range(n_blk):
            rws = slice(r * blk, (r + 1) * blk)
            acc_ref[rws, cols] = y_ref[rws, cols].astype(F32) + jnp.dot(
                hbuf[rws, 0:own_cols], o_tile(j)[...], preferred_element_type=F32)

        @pl.when(j < n_tile - 4)
        def _():
            o_in(j + 4).start()

        @pl.when(j == 0)
        def _():
            pass_on(0)

        @pl.when(j == 1)
        def _():
            oy(1).start()
            share(2)

        @pl.when(j == 5)
        def _():
            pass_on(1)
            load_group(0)
        return carry

    lax.fori_loop(0, n_tile, out_own, 0)

    def add_group(g, tick=None):
        for j in range(n_tile):
            w1_in(g, j).wait()

        def add(j, carry):
            for r in range(n_blk):
                rws = slice(r * blk, (r + 1) * blk)
                acc_ref[rws, at(j, width)] += jnp.dot(
                    hbuf[rws, at(g + n_grp, width)], wbuf[g % 2, at(j, width)], preferred_element_type=F32)
            if tick is not None:
                pl.when(j == n_tile // 2)(tick)
            return carry

        lax.fori_loop(0, n_tile, add, 0)

    load_group(1)
    oy(0).wait_recv()
    add_group(0, lambda: oy(2).start())
    share(3)
    oy(1).wait_recv()
    add_group(1)
    pass_on(2)
    o_last(0).start()

    def caches(c, carry):
        rws = at(c, HEAD_DIM)
        for n in range(heads):
            kst_ref[rws, n, :] = kv_ref[0, n, 0, rws, :]
            vst_ref[rws, n, :] = kv_ref[0, n, 1, rws, :].astype(F32).T.astype(BF16)
        return carry

    lax.fori_loop(0, rows // HEAD_DIM, caches, 0)
    load_group(2)
    o_last(0).wait_recv()
    o_last(1).start()
    pass_on(3)
    oy(2).wait_recv()
    o_last(2).start()
    load_group(3)
    add_group(2)
    for j in range(n_tile):
        w1_in(3, j).wait()

    for r in range(len(tail)):
        if r > 0:
            o_last(r).wait_recv()
        if 0 < r < len(tail) - 2:
            o_last(r + 2).start()

        def finish(j, carry):
            cols = at(j, width)
            total = acc_ref[tail[r], cols] + jnp.dot(hbuf[tail[r], at(2 * n_grp - 1, width)], wbuf[1, at(j, width)],
                                                     preferred_element_type=F32)
            y_ref[tail[r], cols] = total.astype(BF16)
            return carry

        lax.fori_loop(0, n_tile, finish, 0, unroll=4)

    for n in range(4):
        kx(n).wait_send()
        kd(n).wait_send()
        wy(n).wait_send()
        wx(n).wait_send()
        wc(n).wait_send()
        wd(n).wait_send()
    for g in range(3):
        oy(g).wait_send()
    for r in range(len(tail)):
        o_last(r).wait_send()


def write_kernel(y_ref, k_ref, v_ref, y_hbm, k_hbm, v_hbm, sem):
    pieces = 8
    size = y_ref.shape[0] // pieces
    copies = []
    for i in range(pieces):
        part = pl.ds(i * size, size)
        copies.append(pltpu.make_async_copy(y_ref.at[part], y_hbm.at[part], sem.at[i]))
    copies.append(pltpu.make_async_copy(k_ref, k_hbm, sem.at[pieces]))
    copies.append(pltpu.make_async_copy(v_ref, v_hbm, sem.at[pieces + 1]))
    for copy in copies:
        copy.start()
    for copy in copies:
        copy.wait()


def solution(mesh):
    def device_fn(x_in, positions, norm_gain, w_q, w_k, w_v, w_o):
        rows, dim = x_in.shape
        cols = w_k.shape[1]
        kv_dev = cols // HEAD_DIM
        seg = rows // 2
        half = HEAD_DIM // 2
        hbm = pl.BlockSpec(memory_space=pl.ANY)
        vmem = pl.BlockSpec(memory_space=pltpu.VMEM)
        dma = pltpu.SemaphoreType.DMA
        y_raw, k_flat, v_flat, _ = pl.pallas_call(
            layer_kernel,
            in_specs=[hbm] * 8,
            out_specs=[vmem] * 3 + [hbm],
            out_shape=[
                pltpu.VMEM((rows, dim), BF16),
                pltpu.VMEM((rows, kv_dev, HEAD_DIM), BF16),
                pltpu.VMEM((rows, kv_dev, HEAD_DIM), BF16),
                jax.ShapeDtypeStruct(w_o.shape, BF16),
            ],
            scratch_shapes=[
                pltpu.VMEM((rows, dim), BF16),
                pltpu.VMEM((2, dim, cols), BF16),
                pltpu.VMEM((4, kv_dev, 2, rows, HEAD_DIM), BF16),
                pltpu.VMEM((w_q.shape[1], rows), BF16),
                pltpu.VMEM((seg, seg), F32),
                pltpu.VMEM((seg, seg), F32),
                pltpu.VMEM((seg, seg), BF16),
                pltpu.VMEM((seg, seg), BF16),
                pltpu.VMEM((2, 8, seg), F32),
                pltpu.VMEM((2, 8, seg), F32),
                pltpu.VMEM((2, cols, seg), F32),
                pltpu.VMEM((rows, dim), F32),
                pltpu.VMEM((half, rows), F32),
                pltpu.VMEM((half, rows), F32),
                pltpu.VMEM((1, dim), F32),
                pltpu.VMEM((1, rows), jnp.int32),
                pltpu.VMEM((half, 1), F32),
                pltpu.VMEM((dim // HEAD_DIM, HEAD_DIM), BF16),
                dma((4,)), dma((4,)), dma((2, 8)), dma((3,)),
                dma((4,)), dma((4,)), dma((4,)), dma((4,)), dma((4,)), dma((4,)), dma((4,)), dma((4,)),
                dma, dma, dma((4,)), dma((4,)), dma((4,)), dma((4,)),
                dma((3,)), dma((3,)), dma((5,)), dma((5,)),
                pltpu.SemaphoreType.REGULAR,
            ],
            compiler_params=pltpu.CompilerParams(collective_id=0, has_side_effects=True, vmem_limit_bytes=53 * 1024 * 1024),
            name="layer",
        )(x_in, positions.reshape(1, rows), jnp.asarray(rope_freqs())[:, None], norm_gain.reshape(dim // HEAD_DIM, HEAD_DIM), w_q, w_k, w_v, w_o)
        cache = jax.ShapeDtypeStruct((rows, kv_dev, HEAD_DIM), BF16)
        return pl.pallas_call(
            write_kernel,
            in_specs=[vmem] * 3,
            out_specs=[hbm] * 3,
            out_shape=[jax.ShapeDtypeStruct((rows, dim), BF16), cache, cache],
            scratch_shapes=[dma((10,))],
            compiler_params=pltpu.CompilerParams(vmem_limit_bytes=2 * 1024 * 1024),
            name="write",
        )(y_raw, k_flat, v_flat)

    row_spec = P(('dp', 'cp'), None)
    cache_spec = P(('dp', 'cp'), 'tp', None)
    return jax.shard_map(device_fn, mesh=mesh, in_specs=(row_spec, P(('dp', 'cp')), P(None), P(None, 'tp'), P(None, 'tp'), P(None, 'tp'), P('tp', None)), out_specs=(row_spec, cache_spec, cache_spec), check_vma=False)
```

```python
import math
import functools
import numpy as np
import jax
import jax.numpy as jnp
from jax import lax
from jax.experimental import pallas as pl
from jax.experimental.pallas import tpu as pltpu
from jax.sharding import PartitionSpec as P

HEAD_DIM = 128
NORM_EPS = 1e-5
SCALE_LOG2 = (1.0 / math.sqrt(HEAD_DIM)) * math.log2(math.e)
N_CP = 4
MESH = pl.DeviceIdType.MESH
BF16 = jnp.bfloat16
F32 = jnp.float32


def rope_freqs():
    exponent = np.arange(0, HEAD_DIM, 2) / HEAD_DIM
    base_freq = 1.0 / (500000.0 ** exponent)
    wave_len = 2.0 * math.pi / base_freq
    smooth = (8192.0 / wave_len - 1.0) / 3.0
    blended = (1.0 - smooth) * base_freq / 8.0 + smooth * base_freq
    freqs = np.where(wave_len < 2048.0, base_freq, np.where(wave_len > 8192.0, base_freq / 8.0, blended))
    return freqs.astype(np.float32)


def layer_kernel(x_hbm, pos_hbm, freq_hbm, gain_hbm, wq_hbm, wk_hbm, wv_hbm, wo_hbm,
                 y_ref, kst_ref, vst_ref, w1_hbm,
                 hbuf, wbuf, kv_ref, qt_ref, s_even, s_odd, p_even, p_odd,
                 m_ref, l_ref, att_ref, acc_ref, cos_t, sin_t, gain_f, pos_ref, freq_ref, gain_ref,
                 x_sem, w_sem, f_sem, t_sem,
                 wy_s, wy_r, wx_s, wx_r, wc_s, wc_r, wd_s, wd_r,
                 kc_s, kc_r, kx_s, kx_r, kd_s, kd_r, oy_s, oy_r, or_s, or_r, free_sem):
    rows, dim = hbuf.shape
    width = wk_hbm.shape[1]
    n_grp = wq_hbm.shape[1] // width
    own_cols = n_grp * width
    seg = rows // 2
    half = HEAD_DIM // 2
    blk = 256
    n_blk = rows // blk
    heads = width // HEAD_DIM
    me = lax.axis_index("cp")
    peer_y = {"tp": 1 - lax.axis_index("tp")}
    peer_c = {"cp": me + 1 - 2 * (me % 2)}
    peer_x = {"cp": (me + 2) % N_CP}
    s_refs, p_refs = (s_even, s_odd), (p_even, p_odd)

    def at(i, size):
        return pl.ds(pl.multiple_of(i * size, size), size)

    def remote(src, dst, send, recv, peer):
        return pltpu.make_async_remote_copy(src_ref=src, dst_ref=dst, send_sem=send, recv_sem=recv,
                                            device_id=peer, device_id_type=MESH)

    def w_rows(g, owner):
        return pl.ds(pl.multiple_of(g * width + owner * HEAD_DIM, HEAD_DIM), HEAD_DIM)

    other_x = (me + 2) % N_CP

    def wy(g):
        return remote(wo_hbm.at[w_rows(g, me)], w1_hbm.at[w_rows(g, me)], wy_s.at[g], wy_r.at[g], peer_y)

    def wx(g):
        return remote(w1_hbm.at[w_rows(g, me)], w1_hbm.at[w_rows(g, me)], wx_s.at[g], wx_r.at[g], peer_x)

    def wc(g):
        return remote(w1_hbm.at[w_rows(g, me)], w1_hbm.at[w_rows(g, me)], wc_s.at[g], wc_r.at[g], peer_c)

    def wd(g):
        return remote(w1_hbm.at[w_rows(g, other_x)], w1_hbm.at[w_rows(g, other_x)], wd_s.at[g], wd_r.at[g], peer_c)

    def kc():
        return remote(kv_ref.at[0], kv_ref.at[1], kc_s, kc_r, peer_c)

    def kx(n):
        return remote(kv_ref.at[0, n], kv_ref.at[2, n], kx_s.at[n], kx_r.at[n], peer_x)

    def kd(n):
        return remote(kv_ref.at[2, n], kv_ref.at[3, n], kd_s.at[n], kd_r.at[n], peer_c)

    def oy(g):
        return remote(hbuf.at[:, at(g, width)], hbuf.at[:, at(g + n_grp, width)], oy_s.at[g], oy_r.at[g], peer_y)

    tail_rows = (256, 256, 256, 128, 128)
    tail = [pl.ds(sum(tail_rows[:r]), tail_rows[r]) for r in range(len(tail_rows))]

    def o_last(r):
        g = n_grp - 1
        return remote(hbuf.at[tail[r], at(g, width)], hbuf.at[tail[r], at(g + n_grp, width)],
                      or_s.at[r], or_r.at[r], peer_y)

    def x_in(r):
        return pltpu.make_async_copy(x_hbm.at[at(r, blk)], y_ref.at[at(r, blk)], x_sem.at[r])

    def q_in(g):
        return pltpu.make_async_copy(wq_hbm.at[:, at(g, width)], wbuf.at[g % 2], w_sem.at[g % 2])

    def o_tile(j):
        return wbuf.at[(j % 4) // 2, at(j % 2, own_cols)]

    def o_in(j):
        return pltpu.make_async_copy(wo_hbm.at[:, at(j, width)], o_tile(j), w_sem.at[j % 4])

    n_tile = dim // width

    def w1_in(g, j):
        return pltpu.make_async_copy(w1_hbm.at[at(g, width), at(j, width)], wbuf.at[g % 2, at(j, width)], f_sem.at[g % 2, j])

    k_in = pltpu.make_async_copy(wk_hbm, wbuf.at[0], w_sem.at[0])
    v_in = pltpu.make_async_copy(wv_hbm, wbuf.at[1], w_sem.at[1])

    def share(w):
        wy(w).wait_recv()
        wx(w).start()
        wc(w).start()

    def pass_on(w):
        wx(w).wait_recv()
        wd(w).start()

    def load_group(g):
        wc(g).wait_recv()
        wd(g).wait_recv()
        for j in range(n_tile):
            w1_in(g, j).start()

    barrier = pltpu.get_barrier_semaphore()
    for peer in (peer_y, peer_c, peer_x):
        pl.semaphore_signal(barrier, inc=1, device_id=peer, device_id_type=MESH)
    tables = [pltpu.make_async_copy(src, dst, t_sem.at[n])
              for n, (src, dst) in enumerate(((pos_hbm, pos_ref), (freq_hbm, freq_ref), (gain_hbm, gain_ref)))]
    for copy in tables:
        copy.start()
    pl.semaphore_wait(barrier, 3)
    wy(0).start()
    x_in(0).start()
    k_in.start()
    x_in(1).start()
    v_in.start()
    x_in(2).start()
    x_in(3).start()
    for copy in tables:
        copy.wait()
    gain = gain_ref[...].astype(F32)
    gain_f[...] = jnp.concatenate([gain[i:i + 1, :] for i in range(gain.shape[0])], axis=1)

    def trig(c, carry):
        cols = at(c, blk)
        angle = freq_ref[...] * pos_ref[:, cols].astype(F32)
        turns = jnp.floor(angle * (0.5 / math.pi) + 0.5)
        angle = ((angle - turns * 6.28125) - turns * 1.9350051879882812e-03) - turns * 3.0199159819e-07
        cosine, sine = jnp.cos(angle), jnp.sin(angle)
        cos_t[:, cols] = cosine
        sin_t[:, cols] = sine
        full = (at(c % 2, blk), at(c // 2, HEAD_DIM))
        s_even[full] = jnp.concatenate([cosine, cosine], axis=0).T
        s_odd[full] = jnp.concatenate([-sine, sine], axis=0).T
        return carry

    lax.fori_loop(0, n_blk, trig, 0)

    k_in.wait()

    def norm_k(r, carry):
        x_in(r).wait()
        rws = at(r, blk)

        def norm(i, inner):
            part = pl.ds(pl.multiple_of(r * blk + i * 32, 32), 32)
            x = y_ref[part, :].astype(F32)
            normed = x * lax.rsqrt(jnp.mean(x * x, axis=-1, keepdims=True) + NORM_EPS)
            hbuf[part, :] = (normed * gain_f[...]).astype(BF16)
            return inner

        lax.fori_loop(0, blk // 32, norm, 0)
        k = jnp.dot(hbuf[rws, :], wbuf[0], preferred_element_type=F32).astype(BF16)
        full = (at(r % 2, blk), at(r // 2, HEAD_DIM))
        for n in range(heads):
            vec = k[:, n * HEAD_DIM:(n + 1) * HEAD_DIM].astype(F32)
            rot = (vec * s_even[full] + pltpu.roll(vec, half, 1) * s_odd[full]).astype(BF16)
            kv_ref[0, n, 0, rws, :] = rot
        return carry

    lax.fori_loop(0, n_blk, norm_k, 0)
    q_in(0).start()
    v_in.wait()

    def proj_v(r, carry):
        rws = at(r, blk)
        v = jnp.dot(hbuf[rws, :], wbuf[1], preferred_element_type=F32).astype(BF16)
        for n in range(heads):
            for b in range(blk // HEAD_DIM):
                square = v[b * HEAD_DIM:(b + 1) * HEAD_DIM, n * HEAD_DIM:(n + 1) * HEAD_DIM].astype(F32).T.astype(BF16)
                kv_ref[0, n, 1, pl.ds(pl.multiple_of(r * blk + b * HEAD_DIM, HEAD_DIM), HEAD_DIM), :] = square

        @pl.when(r == n_blk - 2)
        def _():
            wy(1).start()
        return carry

    lax.fori_loop(0, n_blk, proj_v, 0)
    q_in(1).start()

    def proj_q(g, carry):
        q_in(g).wait()

        def rows_q(r, inner):
            rws = at(r, blk)
            q = jnp.dot(hbuf[rws, :], wbuf[g % 2], preferred_element_type=F32).astype(BF16)
            for n in range(heads):
                vec = q[:, n * HEAD_DIM:(n + 1) * HEAD_DIM].astype(F32).T
                a, b = vec[:half], vec[half:]
                out = jnp.concatenate([a * cos_t[:, rws] - b * sin_t[:, rws], b * cos_t[:, rws] + a * sin_t[:, rws]], axis=0)
                qt_ref[pl.ds(pl.multiple_of(g * width + n * HEAD_DIM, HEAD_DIM), HEAD_DIM), rws] = out.astype(BF16)

            @pl.when(jnp.logical_and(g == 0, r == 0))
            def _():
                kc().start()
                kx(0).start()

            @pl.when(jnp.logical_and(g == n_grp - 1, r == 2))
            def _():
                wy(2).start()
            return inner

        lax.fori_loop(0, n_blk, rows_q, 0)

        @pl.when(g < n_grp - 2)
        def _():
            q_in(g + 2).start()

        @pl.when(g == 1)
        def _():
            kx(1).start()
        return carry

    lax.fori_loop(0, n_grp, proj_q, 0)
    kx(2).start()
    pl.semaphore_signal(free_sem, inc=1, device_id=peer_y, device_id_type=MESH)
    for j in range(4):
        o_in(j).start()
    kc().wait()

    def attention(g, outer):
        kx(g).wait_recv()
        kd(g).start()

        m_ref[...] = jnp.full_like(m_ref, -1e30)
        l_ref[...] = jnp.zeros_like(l_ref)
        att_ref[...] = jnp.zeros_like(att_ref)

        def scores(q_half, src, k_half, n, slot, diagonal):
            k = kv_ref[src, g, 0, at(k_half, seg), :]
            q = qt_ref[pl.ds(pl.multiple_of(g * width + n * HEAD_DIM, HEAD_DIM), HEAD_DIM), at(q_half, seg)]
            s = jnp.dot(k, q, preferred_element_type=F32)
            if diagonal:
                keep = lax.broadcasted_iota(jnp.int32, (seg, seg), 0) <= lax.broadcasted_iota(jnp.int32, (seg, seg), 1)
                s = jnp.where(keep, s, -1e30)
            s_refs[slot][...] = s
            return jnp.max(s.reshape(seg // 8, 8, seg), axis=0)

        def soften(q_half, n, slot, top):
            chunk = 64
            m_old = m_ref[q_half, n:n + 1, :]
            m_new = jnp.maximum(m_old, jnp.max(top, axis=0, keepdims=True))
            alpha = jnp.exp2((m_old - m_new) * SCALE_LOG2)
            shift = jnp.broadcast_to(m_new * SCALE_LOG2, (8, seg))
            m_ref[q_half, n:n + 1, :] = m_new
            total = jnp.zeros((8, seg), F32)
            for c in range(0, seg, chunk):
                s = s_refs[slot][c:c + chunk, :].reshape(chunk // 8, 8, seg)
                p = jnp.exp2(s * SCALE_LOG2 - shift[None])
                total = total + jnp.sum(p, axis=0)
                p_refs[slot][c:c + chunk, :] = p.reshape(chunk, seg).astype(BF16)
            l_ref[q_half, n:n + 1, :] = l_ref[q_half, n:n + 1, :] * alpha + jnp.sum(total, axis=0, keepdims=True)
            return alpha

        def weigh(q_half, src, k_half, n, slot, alpha):
            v_t = jnp.concatenate([kv_ref[src, g, 1, pl.ds(pl.multiple_of(k_half * seg + b, HEAD_DIM), HEAD_DIM), :]
                                   for b in range(0, seg, HEAD_DIM)], axis=1)
            rws = slice(n * HEAD_DIM, (n + 1) * HEAD_DIM)
            att_ref[q_half, rws, :] = att_ref[q_half, rws, :] * alpha + jnp.dot(
                v_t, p_refs[slot][...], preferred_element_type=F32)

        def block(q_half, src, k_half, top, following):
            previous = None
            for n in range(heads):
                if n + 1 < heads:
                    top_next = scores(q_half, src, k_half, n + 1, (n + 1) % 2, following is None)
                else:
                    top_next = None if following is None else scores(*following, 0, 0, False)
                alpha = soften(q_half, n, n % 2, top)
                if previous is not None:
                    weigh(*previous)
                previous = (q_half, src, k_half, n, n % 2, alpha)
                top = top_next
            weigh(*previous)
            return top

        def place(step):
            src = (step + 1) // 2
            near = 1 - src // 2
            lower = near * (me % 2) + (1 - near) * (me // 2)
            free = (1 - step % 2) * ((step + 6) // 7)
            return 1 - free * lower, src, free * (1 - lower)

        def on_diagonal(side, carry):
            block(side, 0, side, scores(side, 0, side, 0, 0, True), None)
            return carry

        lax.fori_loop(0, 2, on_diagonal, 0)
        kd(g).wait_recv()
        n_steps = 7

        def step_body(step, top):
            @pl.when(jnp.logical_and(g == 0, step == 6))
            def _():
                share(0)

            @pl.when(jnp.logical_and(g == 1, step == 2))
            def _():
                wy(3).start()

            @pl.when(jnp.logical_and(g == 1, step == 3))
            def _():
                kx(3).start()

            @pl.when(jnp.logical_and(g == 2, step == 6))
            def _():
                pl.semaphore_wait(free_sem, 1)
                oy(0).start()
                share(1)

            return block(*place(step), top, place(jnp.minimum(step + 1, n_steps - 1)))

        lax.fori_loop(0, n_steps, step_body, scores(*place(0), 0, 0, False))

        def write(q_half, carry):
            for n in range(heads):
                o = (att_ref[q_half, n * HEAD_DIM:(n + 1) * HEAD_DIM, :] / l_ref[q_half, n:n + 1, :]).T.astype(BF16)
                hbuf[at(q_half, seg), pl.ds(pl.multiple_of(g * width + n * HEAD_DIM, HEAD_DIM), HEAD_DIM)] = o
            return carry

        lax.fori_loop(0, 2, write, 0)
        return outer

    lax.fori_loop(0, n_grp, attention, 0)

    def out_own(j, carry):
        o_in(j).wait()
        cols = at(j, width)
        for r in range(n_blk):
            rws = slice(r * blk, (r + 1) * blk)
            acc_ref[rws, cols] = y_ref[rws, cols].astype(F32) + jnp.dot(
                hbuf[rws, 0:own_cols], o_tile(j)[...], preferred_element_type=F32)

        @pl.when(j < n_tile - 4)
        def _():
            o_in(j + 4).start()

        @pl.when(j == 0)
        def _():
            pass_on(0)

        @pl.when(j == 1)
        def _():
            oy(1).start()
            share(2)

        @pl.when(j == 5)
        def _():
            pass_on(1)
            load_group(0)
        return carry

    lax.fori_loop(0, n_tile, out_own, 0)

    def add_group(g, tick=None):
        for j in range(n_tile):
            w1_in(g, j).wait()

        def add(j, carry):
            for r in range(n_blk):
                rws = slice(r * blk, (r + 1) * blk)
                acc_ref[rws, at(j, width)] += jnp.dot(
                    hbuf[rws, at(g + n_grp, width)], wbuf[g % 2, at(j, width)], preferred_element_type=F32)
            if tick is not None:
                pl.when(j == n_tile // 2)(tick)
            return carry

        lax.fori_loop(0, n_tile, add, 0)

    load_group(1)
    oy(0).wait_recv()
    add_group(0, lambda: oy(2).start())
    share(3)
    oy(1).wait_recv()
    add_group(1)
    pass_on(2)
    for r in range(len(tail)):
        o_last(r).start()

    def caches(c, carry):
        rws = at(c, HEAD_DIM)
        for n in range(heads):
            kst_ref[rws, n, :] = kv_ref[0, n, 0, rws, :]
            vst_ref[rws, n, :] = kv_ref[0, n, 1, rws, :].astype(F32).T.astype(BF16)
        return carry

    lax.fori_loop(0, rows // HEAD_DIM, caches, 0)
    load_group(2)
    pass_on(3)
    oy(2).wait_recv()
    load_group(3)
    add_group(2)
    for j in range(n_tile):
        w1_in(3, j).wait()

    for r in range(len(tail)):
        o_last(r).wait_recv()

        def finish(j, carry):
            cols = at(j, width)
            total = acc_ref[tail[r], cols] + jnp.dot(hbuf[tail[r], at(2 * n_grp - 1, width)], wbuf[1, at(j, width)],
                                                     preferred_element_type=F32)
            y_ref[tail[r], cols] = total.astype(BF16)
            return carry

        lax.fori_loop(0, n_tile, finish, 0, unroll=4)

    for n in range(4):
        kx(n).wait_send()
        kd(n).wait_send()
        wy(n).wait_send()
        wx(n).wait_send()
        wc(n).wait_send()
        wd(n).wait_send()
    for g in range(3):
        oy(g).wait_send()
    for r in range(len(tail)):
        o_last(r).wait_send()


def write_kernel(y_ref, k_ref, v_ref, y_hbm, k_hbm, v_hbm, sem):
    pieces = 8
    size = y_ref.shape[0] // pieces
    copies = []
    for i in range(pieces):
        part = pl.ds(i * size, size)
        copies.append(pltpu.make_async_copy(y_ref.at[part], y_hbm.at[part], sem.at[i]))
    copies.append(pltpu.make_async_copy(k_ref, k_hbm, sem.at[pieces]))
    copies.append(pltpu.make_async_copy(v_ref, v_hbm, sem.at[pieces + 1]))
    for copy in copies:
        copy.start()
    for copy in copies:
        copy.wait()


def solution(mesh):
    def device_fn(x_in, positions, norm_gain, w_q, w_k, w_v, w_o):
        rows, dim = x_in.shape
        cols = w_k.shape[1]
        kv_dev = cols // HEAD_DIM
        seg = rows // 2
        half = HEAD_DIM // 2
        hbm = pl.BlockSpec(memory_space=pl.ANY)
        vmem = pl.BlockSpec(memory_space=pltpu.VMEM)
        dma = pltpu.SemaphoreType.DMA
        y_raw, k_flat, v_flat, _ = pl.pallas_call(
            layer_kernel,
            in_specs=[hbm] * 8,
            out_specs=[vmem] * 3 + [hbm],
            out_shape=[
                pltpu.VMEM((rows, dim), BF16),
                pltpu.VMEM((rows, kv_dev, HEAD_DIM), BF16),
                pltpu.VMEM((rows, kv_dev, HEAD_DIM), BF16),
                jax.ShapeDtypeStruct(w_o.shape, BF16),
            ],
            scratch_shapes=[
                pltpu.VMEM((rows, dim), BF16),
                pltpu.VMEM((2, dim, cols), BF16),
                pltpu.VMEM((4, kv_dev, 2, rows, HEAD_DIM), BF16),
                pltpu.VMEM((w_q.shape[1], rows), BF16),
                pltpu.VMEM((seg, seg), F32),
                pltpu.VMEM((seg, seg), F32),
                pltpu.VMEM((seg, seg), BF16),
                pltpu.VMEM((seg, seg), BF16),
                pltpu.VMEM((2, 8, seg), F32),
                pltpu.VMEM((2, 8, seg), F32),
                pltpu.VMEM((2, cols, seg), F32),
                pltpu.VMEM((rows, dim), F32),
                pltpu.VMEM((half, rows), F32),
                pltpu.VMEM((half, rows), F32),
                pltpu.VMEM((1, dim), F32),
                pltpu.VMEM((1, rows), jnp.int32),
                pltpu.VMEM((half, 1), F32),
                pltpu.VMEM((dim // HEAD_DIM, HEAD_DIM), BF16),
                dma((4,)), dma((4,)), dma((2, 8)), dma((3,)),
                dma((4,)), dma((4,)), dma((4,)), dma((4,)), dma((4,)), dma((4,)), dma((4,)), dma((4,)),
                dma, dma, dma((4,)), dma((4,)), dma((4,)), dma((4,)),
                dma((3,)), dma((3,)), dma((5,)), dma((5,)),
                pltpu.SemaphoreType.REGULAR,
            ],
            compiler_params=pltpu.CompilerParams(collective_id=0, has_side_effects=True, vmem_limit_bytes=53 * 1024 * 1024),
            name="layer",
        )(x_in, positions.reshape(1, rows), jnp.asarray(rope_freqs())[:, None], norm_gain.reshape(dim // HEAD_DIM, HEAD_DIM), w_q, w_k, w_v, w_o)
        cache = jax.ShapeDtypeStruct((rows, kv_dev, HEAD_DIM), BF16)
        return pl.pallas_call(
            write_kernel,
            in_specs=[vmem] * 3,
            out_specs=[hbm] * 3,
            out_shape=[jax.ShapeDtypeStruct((rows, dim), BF16), cache, cache],
            scratch_shapes=[dma((10,))],
            compiler_params=pltpu.CompilerParams(vmem_limit_bytes=2 * 1024 * 1024),
            name="write",
        )(y_raw, k_flat, v_flat)

    row_spec = P(('dp', 'cp'), None)
    cache_spec = P(('dp', 'cp'), 'tp', None)
    return jax.shard_map(device_fn, mesh=mesh, in_specs=(row_spec, P(('dp', 'cp')), P(None), P(None, 'tp'), P(None, 'tp'), P(None, 'tp'), P('tp', None)), out_specs=(row_spec, cache_spec, cache_spec), check_vma=False)
```

```python
import math
import functools
import numpy as np
import jax
import jax.numpy as jnp
from jax import lax
from jax.experimental import pallas as pl
from jax.experimental.pallas import tpu as pltpu
from jax.sharding import PartitionSpec as P

HEAD_DIM = 128
NORM_EPS = 1e-5
SCALE_LOG2 = (1.0 / math.sqrt(HEAD_DIM)) * math.log2(math.e)
N_CP = 4
MESH = pl.DeviceIdType.MESH
BF16 = jnp.bfloat16
F32 = jnp.float32


def rope_freqs():
    exponent = np.arange(0, HEAD_DIM, 2) / HEAD_DIM
    base_freq = 1.0 / (500000.0 ** exponent)
    wave_len = 2.0 * math.pi / base_freq
    smooth = (8192.0 / wave_len - 1.0) / 3.0
    blended = (1.0 - smooth) * base_freq / 8.0 + smooth * base_freq
    freqs = np.where(wave_len < 2048.0, base_freq, np.where(wave_len > 8192.0, base_freq / 8.0, blended))
    return freqs.astype(np.float32)


def layer_kernel(x_hbm, pos_hbm, freq_hbm, gain_hbm, wq_hbm, wk_hbm, wv_hbm, wo_hbm,
                 y_ref, kst_ref, vst_ref, w1_hbm,
                 hbuf, wbuf, kv_ref, qt_ref, s_even, s_odd, p_even, p_odd,
                 m_ref, l_ref, att_ref, acc_ref, cos_t, sin_t, gain_f, pos_ref, freq_ref, gain_ref,
                 x_sem, w_sem, f_sem, t_sem,
                 wy_s, wy_r, wx_s, wx_r, wc_s, wc_r, wd_s, wd_r,
                 kc_s, kc_r, kx_s, kx_r, kd_s, kd_r, oy_s, oy_r, or_s, or_r, free_sem):
    rows, dim = hbuf.shape
    width = wk_hbm.shape[1]
    n_grp = wq_hbm.shape[1] // width
    own_cols = n_grp * width
    seg = rows // 2
    half = HEAD_DIM // 2
    blk = 256
    n_blk = rows // blk
    heads = width // HEAD_DIM
    me = lax.axis_index("cp")
    peer_y = {"tp": 1 - lax.axis_index("tp")}
    peer_c = {"cp": me + 1 - 2 * (me % 2)}
    peer_x = {"cp": (me + 2) % N_CP}
    s_refs, p_refs = (s_even, s_odd), (p_even, p_odd)

    def at(i, size):
        return pl.ds(pl.multiple_of(i * size, size), size)

    def remote(src, dst, send, recv, peer):
        return pltpu.make_async_remote_copy(src_ref=src, dst_ref=dst, send_sem=send, recv_sem=recv,
                                            device_id=peer, device_id_type=MESH)

    def w_rows(g, owner):
        return pl.ds(pl.multiple_of(g * width + owner * HEAD_DIM, HEAD_DIM), HEAD_DIM)

    other_x = (me + 2) % N_CP

    def wy(g):
        return remote(wo_hbm.at[w_rows(g, me)], w1_hbm.at[w_rows(g, me)], wy_s.at[g], wy_r.at[g], peer_y)

    def wx(g):
        return remote(w1_hbm.at[w_rows(g, me)], w1_hbm.at[w_rows(g, me)], wx_s.at[g], wx_r.at[g], peer_x)

    def wc(g):
        return remote(w1_hbm.at[w_rows(g, me)], w1_hbm.at[w_rows(g, me)], wc_s.at[g], wc_r.at[g], peer_c)

    def wd(g):
        return remote(w1_hbm.at[w_rows(g, other_x)], w1_hbm.at[w_rows(g, other_x)], wd_s.at[g], wd_r.at[g], peer_c)

    def kc():
        return remote(kv_ref.at[0], kv_ref.at[1], kc_s, kc_r, peer_c)

    def kx(n):
        return remote(kv_ref.at[0, n], kv_ref.at[2, n], kx_s.at[n], kx_r.at[n], peer_x)

    def kd(n):
        return remote(kv_ref.at[2, n], kv_ref.at[3, n], kd_s.at[n], kd_r.at[n], peer_c)

    def oy(g):
        return remote(hbuf.at[:, at(g, width)], hbuf.at[:, at(g + n_grp, width)], oy_s.at[g], oy_r.at[g], peer_y)

    tail_rows = (256, 256, 256, 128, 128)
    tail = [pl.ds(sum(tail_rows[:r]), tail_rows[r]) for r in range(len(tail_rows))]

    def o_last(r):
        g = n_grp - 1
        return remote(hbuf.at[tail[r], at(g, width)], hbuf.at[tail[r], at(g + n_grp, width)],
                      or_s.at[r], or_r.at[r], peer_y)

    def x_in(r):
        return pltpu.make_async_copy(x_hbm.at[at(r, blk)], y_ref.at[at(r, blk)], x_sem.at[r])

    def q_in(g):
        return pltpu.make_async_copy(wq_hbm.at[:, at(g, width)], wbuf.at[g % 2], w_sem.at[g % 2])

    def o_tile(j):
        return wbuf.at[(j % 4) // 2, at(j % 2, own_cols)]

    def o_in(j):
        return pltpu.make_async_copy(wo_hbm.at[:, at(j, width)], o_tile(j), w_sem.at[j % 4])

    n_tile = dim // width

    def w1_in(g, j):
        return pltpu.make_async_copy(w1_hbm.at[at(g, width), at(j, width)], wbuf.at[g % 2, at(j, width)], f_sem.at[g % 2, j])

    k_in = pltpu.make_async_copy(wk_hbm, wbuf.at[0], w_sem.at[0])
    v_in = pltpu.make_async_copy(wv_hbm, wbuf.at[1], w_sem.at[1])

    def share(w):
        wy(w).wait_recv()
        wx(w).start()
        wc(w).start()

    def pass_on(w):
        wx(w).wait_recv()
        wd(w).start()

    def load_group(g):
        wc(g).wait_recv()
        wd(g).wait_recv()
        for j in range(n_tile):
            w1_in(g, j).start()

    barrier = pltpu.get_barrier_semaphore()
    for peer in (peer_y, peer_c, peer_x):
        pl.semaphore_signal(barrier, inc=1, device_id=peer, device_id_type=MESH)
    tables = [pltpu.make_async_copy(src, dst, t_sem.at[n])
              for n, (src, dst) in enumerate(((pos_hbm, pos_ref), (freq_hbm, freq_ref), (gain_hbm, gain_ref)))]
    for copy in tables:
        copy.start()
    pl.semaphore_wait(barrier, 3)
    wy(0).start()
    x_in(0).start()
    k_in.start()
    x_in(1).start()
    v_in.start()
    x_in(2).start()
    x_in(3).start()
    for copy in tables:
        copy.wait()
    gain = gain_ref[...].astype(F32)
    gain_f[...] = jnp.concatenate([gain[i:i + 1, :] for i in range(gain.shape[0])], axis=1)

    def trig(c, carry):
        cols = at(c, blk)
        angle = freq_ref[...] * pos_ref[:, cols].astype(F32)
        turns = jnp.floor(angle * (0.5 / math.pi) + 0.5)
        angle = ((angle - turns * 6.28125) - turns * 1.9350051879882812e-03) - turns * 3.0199159819e-07
        cosine, sine = jnp.cos(angle), jnp.sin(angle)
        cos_t[:, cols] = cosine
        sin_t[:, cols] = sine
        full = (at(c % 2, blk), at(c // 2, HEAD_DIM))
        s_even[full] = jnp.concatenate([cosine, cosine], axis=0).T
        s_odd[full] = jnp.concatenate([-sine, sine], axis=0).T
        return carry

    lax.fori_loop(0, n_blk, trig, 0)

    k_in.wait()

    def norm_k(r, carry):
        x_in(r).wait()
        rws = at(r, blk)

        def norm(i, inner):
            part = pl.ds(pl.multiple_of(r * blk + i * 32, 32), 32)
            x = y_ref[part, :].astype(F32)
            normed = x * lax.rsqrt(jnp.mean(x * x, axis=-1, keepdims=True) + NORM_EPS)
            hbuf[part, :] = (normed * gain_f[...]).astype(BF16)
            return inner

        lax.fori_loop(0, blk // 32, norm, 0)
        k = jnp.dot(hbuf[rws, :], wbuf[0], preferred_element_type=F32).astype(BF16)
        full = (at(r % 2, blk), at(r // 2, HEAD_DIM))
        for n in range(heads):
            vec = k[:, n * HEAD_DIM:(n + 1) * HEAD_DIM].astype(F32)
            rot = (vec * s_even[full] + pltpu.roll(vec, half, 1) * s_odd[full]).astype(BF16)
            kv_ref[0, n, 0, rws, :] = rot
        return carry

    lax.fori_loop(0, n_blk, norm_k, 0)
    q_in(0).start()
    v_in.wait()

    def proj_v(r, carry):
        rws = at(r, blk)
        v = jnp.dot(hbuf[rws, :], wbuf[1], preferred_element_type=F32).astype(BF16)
        for n in range(heads):
            for b in range(blk // HEAD_DIM):
                square = v[b * HEAD_DIM:(b + 1) * HEAD_DIM, n * HEAD_DIM:(n + 1) * HEAD_DIM].astype(F32).T.astype(BF16)
                kv_ref[0, n, 1, pl.ds(pl.multiple_of(r * blk + b * HEAD_DIM, HEAD_DIM), HEAD_DIM), :] = square

        @pl.when(r == n_blk - 2)
        def _():
            wy(1).start()
        return carry

    lax.fori_loop(0, n_blk, proj_v, 0)
    q_in(1).start()

    def proj_q(g, carry):
        q_in(g).wait()

        def rows_q(r, inner):
            rws = at(r, blk)
            q = jnp.dot(hbuf[rws, :], wbuf[g % 2], preferred_element_type=F32).astype(BF16)
            for n in range(heads):
                vec = q[:, n * HEAD_DIM:(n + 1) * HEAD_DIM].astype(F32).T
                a, b = vec[:half], vec[half:]
                out = jnp.concatenate([a * cos_t[:, rws] - b * sin_t[:, rws], b * cos_t[:, rws] + a * sin_t[:, rws]], axis=0)
                qt_ref[pl.ds(pl.multiple_of(g * width + n * HEAD_DIM, HEAD_DIM), HEAD_DIM), rws] = out.astype(BF16)

            @pl.when(jnp.logical_and(g == 0, r == 0))
            def _():
                kc().start()
                kx(0).start()

            @pl.when(jnp.logical_and(g == n_grp - 1, r == 2))
            def _():
                wy(2).start()
            return inner

        lax.fori_loop(0, n_blk, rows_q, 0)

        @pl.when(g < n_grp - 2)
        def _():
            q_in(g + 2).start()

        @pl.when(g == 1)
        def _():
            kx(1).start()
        return carry

    lax.fori_loop(0, n_grp, proj_q, 0)
    kx(2).start()
    pl.semaphore_signal(free_sem, inc=1, device_id=peer_y, device_id_type=MESH)
    for j in range(4):
        o_in(j).start()
    kc().wait()

    def attention(g, outer):
        kx(g).wait_recv()
        kd(g).start()

        m_ref[...] = jnp.full_like(m_ref, -1e30)
        l_ref[...] = jnp.zeros_like(l_ref)
        att_ref[...] = jnp.zeros_like(att_ref)

        def scores(q_half, src, k_half, n, slot, diagonal):
            k = kv_ref[src, g, 0, at(k_half, seg), :]
            q = qt_ref[pl.ds(pl.multiple_of(g * width + n * HEAD_DIM, HEAD_DIM), HEAD_DIM), at(q_half, seg)]
            s = jnp.dot(k, q, preferred_element_type=F32)
            if diagonal:
                keep = lax.broadcasted_iota(jnp.int32, (seg, seg), 0) <= lax.broadcasted_iota(jnp.int32, (seg, seg), 1)
                s = jnp.where(keep, s, -1e30)
            s_refs[slot][...] = s
            return jnp.max(s.reshape(seg // 8, 8, seg), axis=0)

        def soften(q_half, n, slot, top):
            chunk = 64
            m_old = m_ref[q_half, n:n + 1, :]
            m_new = jnp.maximum(m_old, jnp.max(top, axis=0, keepdims=True))
            alpha = jnp.exp2((m_old - m_new) * SCALE_LOG2)
            shift = jnp.broadcast_to(m_new * SCALE_LOG2, (8, seg))
            m_ref[q_half, n:n + 1, :] = m_new
            total = jnp.zeros((8, seg), F32)
            for c in range(0, seg, chunk):
                s = s_refs[slot][c:c + chunk, :].reshape(chunk // 8, 8, seg)
                p = jnp.exp2(s * SCALE_LOG2 - shift[None])
                total = total + jnp.sum(p, axis=0)
                p_refs[slot][c:c + chunk, :] = p.reshape(chunk, seg).astype(BF16)
            l_ref[q_half, n:n + 1, :] = l_ref[q_half, n:n + 1, :] * alpha + jnp.sum(total, axis=0, keepdims=True)
            return alpha

        def weigh(q_half, src, k_half, n, slot, alpha):
            v_t = jnp.concatenate([kv_ref[src, g, 1, pl.ds(pl.multiple_of(k_half * seg + b, HEAD_DIM), HEAD_DIM), :]
                                   for b in range(0, seg, HEAD_DIM)], axis=1)
            rws = slice(n * HEAD_DIM, (n + 1) * HEAD_DIM)
            att_ref[q_half, rws, :] = att_ref[q_half, rws, :] * alpha + jnp.dot(
                v_t, p_refs[slot][...], preferred_element_type=F32)

        def block(q_half, src, k_half, top, following):
            previous = None
            for n in range(heads):
                if n + 1 < heads:
                    top_next = scores(q_half, src, k_half, n + 1, (n + 1) % 2, following is None)
                else:
                    top_next = None if following is None else scores(*following, 0, 0, False)
                alpha = soften(q_half, n, n % 2, top)
                if previous is not None:
                    weigh(*previous)
                previous = (q_half, src, k_half, n, n % 2, alpha)
                top = top_next
            weigh(*previous)
            return top

        def place(step):
            src = (step + 1) // 2
            near = 1 - src // 2
            lower = near * (me % 2) + (1 - near) * (me // 2)
            free = (1 - step % 2) * ((step + 6) // 7)
            return 1 - free * lower, src, free * (1 - lower)

        def on_diagonal(side, carry):
            block(side, 0, side, scores(side, 0, side, 0, 0, True), None)
            return carry

        lax.fori_loop(0, 2, on_diagonal, 0)
        kd(g).wait_recv()
        n_steps = 7

        def step_body(step, top):
            @pl.when(jnp.logical_and(g == 0, step == 6))
            def _():
                share(0)

            @pl.when(jnp.logical_and(g == 1, step == 2))
            def _():
                wy(3).start()

            @pl.when(jnp.logical_and(g == 1, step == 3))
            def _():
                kx(3).start()

            @pl.when(jnp.logical_and(g == 2, step == 6))
            def _():
                pl.semaphore_wait(free_sem, 1)
                oy(0).start()
                share(1)

            return block(*place(step), top, place(jnp.minimum(step + 1, n_steps - 1)))

        lax.fori_loop(0, n_steps, step_body, scores(*place(0), 0, 0, False))

        def write(q_half, carry):
            for n in range(heads):
                o = (att_ref[q_half, n * HEAD_DIM:(n + 1) * HEAD_DIM, :] / l_ref[q_half, n:n + 1, :]).T.astype(BF16)
                hbuf[at(q_half, seg), pl.ds(pl.multiple_of(g * width + n * HEAD_DIM, HEAD_DIM), HEAD_DIM)] = o
            return carry

        lax.fori_loop(0, 2, write, 0)
        return outer

    lax.fori_loop(0, n_grp, attention, 0)

    def out_own(j, carry):
        o_in(j).wait()
        cols = at(j, width)
        for r in range(n_blk):
            rws = slice(r * blk, (r + 1) * blk)
            acc_ref[rws, cols] = y_ref[rws, cols].astype(F32) + jnp.dot(
                hbuf[rws, 0:own_cols], o_tile(j)[...], preferred_element_type=F32)

        @pl.when(j < n_tile - 4)
        def _():
            o_in(j + 4).start()

        @pl.when(j == 0)
        def _():
            pass_on(0)

        @pl.when(j == 1)
        def _():
            oy(1).start()
            share(2)

        @pl.when(j == 5)
        def _():
            pass_on(1)
            load_group(0)
        return carry

    lax.fori_loop(0, n_tile, out_own, 0)

    def add_group(g, tick=None):
        for j in range(n_tile):
            w1_in(g, j).wait()

        def add(j, carry):
            for r in range(n_blk):
                rws = slice(r * blk, (r + 1) * blk)
                acc_ref[rws, at(j, width)] += jnp.dot(
                    hbuf[rws, at(g + n_grp, width)], wbuf[g % 2, at(j, width)], preferred_element_type=F32)
            if tick is not None:
                pl.when(j == n_tile // 2)(tick)
            return carry

        lax.fori_loop(0, n_tile, add, 0)

    load_group(1)
    oy(0).wait_recv()
    add_group(0, lambda: oy(2).start())
    share(3)
    oy(1).wait_recv()
    add_group(1)
    pass_on(2)
    for r in range(len(tail)):
        o_last(r).start()

    def caches(c, carry):
        rws = at(c, HEAD_DIM)
        for n in range(heads):
            kst_ref[rws, n, :] = kv_ref[0, n, 0, rws, :]
            vst_ref[rws, n, :] = kv_ref[0, n, 1, rws, :].astype(F32).T.astype(BF16)
        return carry

    lax.fori_loop(0, rows // HEAD_DIM, caches, 0)
    load_group(2)
    pass_on(3)
    oy(2).wait_recv()
    load_group(3)
    add_group(2)
    for j in range(n_tile):
        w1_in(3, j).wait()

    for n in range(4):
        for copy in (kx, kd, wy, wx, wc, wd):
            copy(n).wait_send()
    for g in range(n_grp - 1):
        oy(g).wait_send()

    for r in range(len(tail)):
        o_last(r).wait_recv()

        def finish(j, carry):
            cols = at(j, width)
            total = acc_ref[tail[r], cols] + jnp.dot(hbuf[tail[r], at(2 * n_grp - 1, width)], wbuf[1, at(j, width)],
                                                     preferred_element_type=F32)
            y_ref[tail[r], cols] = total.astype(BF16)
            return carry

        lax.fori_loop(0, n_tile, finish, 0, unroll=True)

    for r in range(len(tail)):
        o_last(r).wait_send()


def write_kernel(y_ref, k_ref, v_ref, y_hbm, k_hbm, v_hbm, sem):
    pieces = 8
    size = y_ref.shape[0] // pieces
    copies = []
    for i in range(pieces):
        part = pl.ds(i * size, size)
        copies.append(pltpu.make_async_copy(y_ref.at[part], y_hbm.at[part], sem.at[i]))
    copies.append(pltpu.make_async_copy(k_ref, k_hbm, sem.at[pieces]))
    copies.append(pltpu.make_async_copy(v_ref, v_hbm, sem.at[pieces + 1]))
    for copy in copies:
        copy.start()
    for copy in copies:
        copy.wait()


def solution(mesh):
    def device_fn(x_in, positions, norm_gain, w_q, w_k, w_v, w_o):
        rows, dim = x_in.shape
        cols = w_k.shape[1]
        kv_dev = cols // HEAD_DIM
        seg = rows // 2
        half = HEAD_DIM // 2
        hbm = pl.BlockSpec(memory_space=pl.ANY)
        vmem = pl.BlockSpec(memory_space=pltpu.VMEM)
        dma = pltpu.SemaphoreType.DMA
        y_raw, k_flat, v_flat, _ = pl.pallas_call(
            layer_kernel,
            in_specs=[hbm] * 8,
            out_specs=[vmem] * 3 + [hbm],
            out_shape=[
                pltpu.VMEM((rows, dim), BF16),
                pltpu.VMEM((rows, kv_dev, HEAD_DIM), BF16),
                pltpu.VMEM((rows, kv_dev, HEAD_DIM), BF16),
                jax.ShapeDtypeStruct(w_o.shape, BF16),
            ],
            scratch_shapes=[
                pltpu.VMEM((rows, dim), BF16),
                pltpu.VMEM((2, dim, cols), BF16),
                pltpu.VMEM((4, kv_dev, 2, rows, HEAD_DIM), BF16),
                pltpu.VMEM((w_q.shape[1], rows), BF16),
                pltpu.VMEM((seg, seg), F32),
                pltpu.VMEM((seg, seg), F32),
                pltpu.VMEM((seg, seg), BF16),
                pltpu.VMEM((seg, seg), BF16),
                pltpu.VMEM((2, 8, seg), F32),
                pltpu.VMEM((2, 8, seg), F32),
                pltpu.VMEM((2, cols, seg), F32),
                pltpu.VMEM((rows, dim), F32),
                pltpu.VMEM((half, rows), F32),
                pltpu.VMEM((half, rows), F32),
                pltpu.VMEM((1, dim), F32),
                pltpu.VMEM((1, rows), jnp.int32),
                pltpu.VMEM((half, 1), F32),
                pltpu.VMEM((dim // HEAD_DIM, HEAD_DIM), BF16),
                dma((4,)), dma((4,)), dma((2, 8)), dma((3,)),
                dma((4,)), dma((4,)), dma((4,)), dma((4,)), dma((4,)), dma((4,)), dma((4,)), dma((4,)),
                dma, dma, dma((4,)), dma((4,)), dma((4,)), dma((4,)),
                dma((3,)), dma((3,)), dma((5,)), dma((5,)),
                pltpu.SemaphoreType.REGULAR,
            ],
            compiler_params=pltpu.CompilerParams(collective_id=0, has_side_effects=True, vmem_limit_bytes=53 * 1024 * 1024),
            name="layer",
        )(x_in, positions.reshape(1, rows), jnp.asarray(rope_freqs())[:, None], norm_gain.reshape(dim // HEAD_DIM, HEAD_DIM), w_q, w_k, w_v, w_o)
        cache = jax.ShapeDtypeStruct((rows, kv_dev, HEAD_DIM), BF16)
        return pl.pallas_call(
            write_kernel,
            in_specs=[vmem] * 3,
            out_specs=[hbm] * 3,
            out_shape=[jax.ShapeDtypeStruct((rows, dim), BF16), cache, cache],
            scratch_shapes=[dma((10,))],
            compiler_params=pltpu.CompilerParams(vmem_limit_bytes=2 * 1024 * 1024),
            name="write",
        )(y_raw, k_flat, v_flat)

    row_spec = P(('dp', 'cp'), None)
    cache_spec = P(('dp', 'cp'), 'tp', None)
    return jax.shard_map(device_fn, mesh=mesh, in_specs=(row_spec, P(('dp', 'cp')), P(None), P(None, 'tp'), P(None, 'tp'), P(None, 'tp'), P('tp', None)), out_specs=(row_spec, cache_spec, cache_spec), check_vma=False)
```
